32 devices in a mesh: slab: 16 (over z, y, x), sub: 2 (over core).
Axes of the slice: x: 2, y: 2, z: 4, core: 2. Of those that a mesh axis runs over, the one named last changes fastest.
Arguments:
- start: float32 [4, 96, 32, 256], P(None, 'slab', 'sub'), may hold values from -6 to 6
- wind: float32 [3, 96, 32, 256], P(None, 'slab', 'sub'), may hold values from -4 to 4
- reaction: float32 [96, 32, 256], P('slab', 'sub'), may hold values from 0.5 to 4
- mass: float32 [96, 32, 256], P('slab', 'sub'), may hold values from 0.5 to 2
Outputs:
- basis: float32 [4, 4, 96, 32, 256], P(None, None, 'slab', 'sub')
- search: float32 [3, 4, 96, 32, 256], P(None, None, 'slab', 'sub')
- hessenberg: float32 [4, 3], replicated
The draws below stay inside these ranges and needn't reach their ends.
All inputs are finite; a program needn't handle non-finite values.
Results may differ from the reference program's by a relative error of at most 0.0003.
Values sent between devices are 32-bit elements; how exact they have to be, the bound alone decides.
A program may use at most 64 MiB of HBM per device.

```python
import math
import jax
import jax.numpy as jnp

NZ = 256
ITERS = 3
NX = 96
NY = 32


def level_of(key, shape, split, low, top_value):
    loudness, own = 1.0, jax.random.fold_in(key, 6)
    for axis_at, blocks in split:
        draws = jnp.exp(jax.random.uniform(jax.random.fold_in(own, axis_at), (blocks,), jnp.float32, low / len(split), top_value / len(split)))
        loudness = loudness * jnp.repeat(draws, shape[axis_at] // blocks).reshape([-1 if axis == axis_at else 1 for axis in range(len(shape))])
    return loudness


def normal_values(own_key, shape, spread, reach, split=(), held_as=jnp.bfloat16):
    loudness = level_of(own_key, shape, split, -0.22, 0.18) if split else 1.0
    values = jax.random.normal(own_key, shape, jnp.float32) * spread * loudness
    return jnp.minimum(jnp.maximum(values, -reach), reach).astype(held_as)


def setup_inputs(seed: int = 0) -> dict:
    splits = jax.random.split(jax.random.key(seed), 5)
    return {
        "start": normal_values(splits[0], (4, NX, NY, NZ), 1.0, 6.0, ((1, 16), (2, 2)), jnp.float32),
        "wind": normal_values(splits[1], (3, NX, NY, NZ), 1.0, 4.0, ((1, 16), (2, 2)), jnp.float32),
        "reaction": jnp.clip(jnp.exp(math.log(4.0) - 2.0794415 * jax.random.uniform(splits[2], (NX, NY, NZ), jnp.float32) ** level_of(splits[2], (NX, NY, NZ), ((0, 16), (1, 2)), -0.2, 0.2)), 0.5, 4.0),
        "mass": jnp.clip(jnp.exp(math.log(2.0) - 1.3862944 * jax.random.uniform(splits[3], (NX, NY, NZ), jnp.float32) ** level_of(splits[3], (NX, NY, NZ), ((0, 16), (1, 2)), -0.2, 0.2)), 0.5, 2.0),
    }


def grid_pad(field):
    return jnp.pad(field, [(0, 0)] * (field.ndim - 3) + [(1, 1), (1, 1), (0, 0)])

def neighbour_sets(padded):
    center = padded[..., 1:-1, 1:-1, :]
    zero_face = jnp.zeros_like(center[..., :1])
    plus_side = (padded[..., 2:, 1:-1, :], padded[..., 1:-1, 2:, :], jnp.concatenate([center[..., 1:], zero_face], -1))
    minus_side = (padded[..., :-2, 1:-1, :], padded[..., 1:-1, :-2, :], jnp.concatenate([zero_face, center[..., :-1]], -1))
    return (center, plus_side, minus_side)

def six_sum(plus_side, minus_side):
    total = plus_side[0] + minus_side[0]
    total = total + plus_side[1] + minus_side[1]
    return total + plus_side[2] + minus_side[2]

def transport(padded, reaction_k, wind_k):
    center, plus_side, minus_side = neighbour_sets(padded)
    convect = wind_k[0] * (plus_side[0] - minus_side[0])
    convect = convect + wind_k[1] * (plus_side[1] - minus_side[1])
    convect = convect + wind_k[2] * (plus_side[2] - minus_side[2])
    return (6.0 + reaction_k) * center - six_sum(plus_side, minus_side) + 0.5 * convect

def gradient(padded):
    center, plus_side, minus_side = neighbour_sets(padded)
    return jnp.stack([0.5 * (plus_side[dim_index] - minus_side[dim_index]) for dim_index in range(3)])

def divergence(padded):
    center, plus_side, minus_side = neighbour_sets(padded)
    total = 0.5 * (plus_side[0][0] - minus_side[0][0])
    total = total + 0.5 * (plus_side[1][1] - minus_side[1][1])
    return total + 0.5 * (plus_side[2][2] - minus_side[2][2])

def pressure_poisson(padded):
    center, plus_side, minus_side = neighbour_sets(padded)
    return 7.0 * center - six_sum(plus_side, minus_side)

def oseen_apply(padded, reaction_k, wind_k):
    upper = transport(padded[:3], reaction_k, wind_k) + gradient(padded[3])
    center, plus_side, minus_side = neighbour_sets(padded[3])
    lower = -divergence(padded[:3]) - 0.5 * (6.0 * center - six_sum(plus_side, minus_side))
    return jnp.concatenate([upper, lower[None]], 0)

def precondition(vector, wind, reaction, mass):
    pressure = vector[3]
    first_guess = pressure / 7.0
    second_guess = first_guess + (pressure - pressure_poisson(grid_pad(first_guess))) / 7.0
    schur = -transport(grid_pad(second_guess), reaction, wind) / mass
    residue = vector[:3] - gradient(grid_pad(schur))
    diagonal = 6.0 + reaction
    velocity_first = residue / diagonal
    velocity = velocity_first + (residue - transport(grid_pad(velocity_first), reaction, wind)) / diagonal
    return jnp.concatenate([velocity, schur[None]], 0)

def reference(start, wind, reaction, mass):
    scale_start = jnp.sqrt(jnp.sum(start * start))
    vectors = [start / scale_start]
    searches = []
    hess = jnp.zeros((ITERS + 1, ITERS), jnp.float32)
    for column in range(ITERS):
        found = precondition(vectors[column], wind, reaction, mass)
        searches.append(found)
        image = oseen_apply(grid_pad(found), reaction, wind)
        projected = jnp.stack([jnp.sum(vectors[row] * image) for row in range(column + 1)])
        for row in range(column + 1):
            image = image - projected[row] * vectors[row]
        norm_next = jnp.sqrt(jnp.sum(image * image))
        hess = hess.at[:column + 1, column].set(projected)
        hess = hess.at[column + 1, column].set(norm_next)
        vectors.append(image / norm_next)
    return (jnp.stack(vectors), jnp.stack(searches), hess)
```

```python
import functools

import jax
import jax.numpy as jnp
from jax import lax
from jax.experimental import pallas as pl
from jax.experimental.pallas import tpu as pltpu
from jax.sharding import PartitionSpec as P

ITERS = 3
UNROLL = 3
LANES = 128
MESH = pl.DeviceIdType.MESH


def fold(x):
    rows, cols = x.shape
    total = None
    for r in range(0, rows, 8):
        for c in range(0, cols, LANES):
            piece = x[r : r + 8, c : c + LANES]
            total = piece if total is None else total + piece
    return total


def loop(count, body, init=0, low=0):
    step = max(u for u in range(1, UNROLL + 1) if count % u == 0)

    def several(k, carry):
        for i in range(step):
            carry = body(low + k * step + i, carry)
        return carry

    return lax.fori_loop(0, count // step, several, init)


def kernel(
    slabs, subs, cx, cy, nz,
    start, wind, reaction, mass, ob, os_, scal,
    stage, xp, xu, qs, y0, t1, z1, raw, co, mk, vv, ss, wl, red,
    init_send, init_recv, send, recv, red_send, red_recv, load, out_local, out_send, out_recv,
):
    slab, sub = lax.axis_index("slab"), lax.axis_index("sub")
    n = slabs * subs
    me = slab * subs + sub
    h = cx // subs
    rows = subs * cy
    f32 = jnp.float32
    other = 1 - sub
    has_left, has_right = me > 0, me < n - 1
    has_cross = jnp.where(sub == 0, slab, slabs - 1 - slab) > 0
    mine = pl.ds(pl.multiple_of(sub * cy, 8), cy)
    theirs = pl.ds(pl.multiple_of(other * cy, 8), cy)

    def staged(lo, count):
        return lambda planes: stage.at[pl.ds(lo, count), planes]

    first = [
        (lambda planes: stage.at[3, planes], lambda planes, lines: xp.at[0, planes, lines], 2, 2),
        (staged(4, 4), lambda planes, lines: raw.at[pl.ds(0, 4), planes, lines], 1, 1),
        (lambda planes: stage.at[8, planes], lambda planes, lines: raw.at[4, planes, lines], 1, 0),
        (staged(0, 3), lambda planes, lines: xu.at[0, :, planes, lines], 1, 1),
    ]

    def window(g, side):
        _, _, at, w = first[g]
        return pl.ds(side * (h - w), h + w), pl.ds(at - side * w, h + w)

    def local(g, src, dst, sem):
        a, b = window(g, sub)
        return pltpu.make_async_copy(src(a), dst(b), load.at[sem])

    stages = [
        pltpu.make_async_copy(start.at[3], stage.at[3], load.at[0]),
        pltpu.make_async_copy(wind, stage.at[pl.ds(4, 3)], load.at[1]),
        pltpu.make_async_copy(reaction, stage.at[7], load.at[2]),
        pltpu.make_async_copy(mass, stage.at[8], load.at[3]),
        pltpu.make_async_copy(start.at[pl.ds(0, 3)], stage.at[pl.ds(0, 3)], load.at[4]),
    ]
    own = [
        local(0, lambda a: start.at[3, a], lambda b: xp.at[0, b, mine], 5),
        local(1, lambda a: wind.at[:, a], lambda b: raw.at[pl.ds(0, 3), b, mine], 6),
        local(1, lambda a: reaction.at[a], lambda b: raw.at[3, b, mine], 7),
        local(2, lambda a: mass.at[a], lambda b: raw.at[4, b, mine], 8),
        local(3, lambda a: start.at[pl.ds(0, 3), a], lambda b: xu.at[0, :, b, mine], 9),
    ]
    first_out = pltpu.make_async_copy(start, ob.at[0], load.at[10])
    for item in stages:
        item.start()
    for item in own:
        item.start()
    first_out.start()

    barrier = pltpu.get_barrier_semaphore()

    def greet(k, carry):
        for core in range(subs):
            pl.semaphore_signal(
                barrier, inc=1, device_id=(lax.rem(slab + k, slabs), core), device_id_type=MESH
            )
        return carry

    pl.semaphore_signal(barrier, inc=1, device_id=(slab, other), device_id_type=MESH)
    lax.fori_loop(1, slabs, greet, 0)

    def clear(low):
        def inner():
            zero = jnp.zeros((rows, nz), f32)
            for e in range(ITERS):
                for k in range(2):
                    at = k if low else 2 + h + k
                    xp[e, at] = zero
                    qs[e, at] = zero
                for c in range(3):
                    xu[e, c, 0 if low else 1 + h] = zero
                    y0[e, c, 0 if low else 3 + h] = zero
            for c in range(4):
                raw[c, 0 if low else 1 + h] = zero
        return inner

    pl.when(jnp.logical_not(has_left))(clear(True))
    pl.when(jnp.logical_not(has_right))(clear(False))

    row = lax.broadcasted_iota(jnp.int32, (rows, nz), 0)
    col = lax.broadcasted_iota(jnp.int32, (rows, nz), 1)
    mk[0] = jnp.where(row == rows - 1, 0.0, 1.0)
    mk[1] = jnp.where(row == 0, 0.0, 1.0)
    mk[2] = jnp.where(col == nz - 1, 0.0, 1.0)
    mk[3] = jnp.where(col == 0, 0.0, 1.0)

    def first_copy(g, kind):
        src, dst, at, w = first[g]
        if kind == 0:
            a, b = window(g, other)
            target, slot = (slab, other), 0
        elif kind == 1:
            a, b = pl.ds(cx - w, w), pl.ds(at - w, w)
            target, slot = (slab + 1, 0), 1 + sub
        else:
            a, b = pl.ds(0, w), pl.ds(at + h, w)
            target, slot = (slab - 1, subs - 1), 1 + sub
        return pltpu.make_async_remote_copy(
            src_ref=src(a), dst_ref=dst(b, mine), send_sem=init_send.at[g, kind],
            recv_sem=init_recv.at[g, slot], device_id=target, device_id_type=MESH,
        )

    def first_begin(g):
        if first[g][3] > 0:
            pl.when(slab < slabs - 1)(lambda: first_copy(g, 1).start())
            pl.when(slab > 0)(lambda: first_copy(g, 2).start())

    def first_wait(ref, sem):
        pltpu.make_async_copy(ref, ref, sem).wait()

    def first_near(g):
        _, dst, _, _ = first[g]
        _, b = window(g, sub)
        first_wait(dst(b, theirs), init_recv.at[g, 0])

    def first_far(g):
        _, dst, at, w = first[g]
        if w > 0:
            def inner():
                for r in range(subs):
                    first_wait(dst(pl.ds(0, w), pl.ds(r * cy, cy)), init_recv.at[g, 1 + r])
            pl.when(has_cross)(inner)

    def first_finish(g):
        first_copy(g, 0).wait_send()
        if first[g][3] > 0:
            pl.when(slab < slabs - 1)(lambda: first_copy(g, 1).wait_send())
            pl.when(slab > 0)(lambda: first_copy(g, 2).wait_send())

    def remote(kind, e, way):
        if kind == 0 or kind == 2:
            ref = (xp, None, qs)[kind].at[e]
            pair = (pl.ds(h, 2), pl.ds(0, 2)) if way == 0 else (pl.ds(2, 2), pl.ds(h + 2, 2))
            src, dst = ref.at[pair[0]], ref.at[pair[1]]
        elif kind == 1:
            pair = (h, 0) if way == 0 else (1, h + 1)
            src, dst = xu.at[e, :, pair[0]], xu.at[e, :, pair[1]]
        else:
            pair = (h, 0) if way == 0 else (3, h + 3)
            src, dst = y0.at[e, :, pair[0]], y0.at[e, :, pair[1]]
        target = me + 1 if way == 0 else me - 1
        return pltpu.make_async_remote_copy(
            src_ref=src, dst_ref=dst, send_sem=send.at[kind, e, way], recv_sem=recv.at[kind, e, way],
            device_id=(target // subs, lax.rem(target, subs)), device_id_type=MESH,
        )

    def begin(kind, e):
        pl.when(has_right)(lambda: remote(kind, e, 0).start())
        pl.when(has_left)(lambda: remote(kind, e, 1).start())

    def arrive(kind, e):
        pl.when(has_left)(lambda: remote(kind, e, 0).wait_recv())
        pl.when(has_right)(lambda: remote(kind, e, 1).wait_recv())

    def finish(kind, e):
        pl.when(has_right)(lambda: remote(kind, e, 0).wait_send())
        pl.when(has_left)(lambda: remote(kind, e, 1).wait_send())

    lane = lax.broadcasted_iota(jnp.int32, (1, LANES), 1)

    def reduce_start(e, parts):
        line = jnp.zeros((1, LANES), f32)
        for i, part in enumerate(parts):
            line = line + jnp.where(lane == i, jnp.sum(fold(part), keepdims=True), 0.0)
        red[e, me] = line

        def tell(at, core):
            pltpu.make_async_remote_copy(
                src_ref=red.at[e, me], dst_ref=red.at[e, me],
                send_sem=red_send.at[e], recv_sem=red_recv.at[e],
                device_id=(at, core), device_id_type=MESH,
            ).start()

        def push(k, carry):
            at = lax.rem(slab + k, slabs)
            for core in range(subs):
                tell(at, core)
            return carry

        lax.fori_loop(1, slabs, push, 0)
        tell(slab, other)

    def red_wait(e, sem):
        block = red.at[e, pl.ds(0, n - 1)]
        pltpu.make_async_copy(block, block, sem.at[e]).wait()

    def reduce_end(e, count):
        red_wait(e, red_recv)
        total = jnp.sum(red[e], axis=0)
        return [
            jnp.sum(jnp.where(lane == i, total, 0.0), axis=1, keepdims=True)
            for i in range(count)
        ]

    def deliver(i, src, dst):
        planes = pl.ds(sub * h, h)
        return (
            pltpu.make_async_copy(src.at[:, :, mine], dst.at[:, planes], out_local.at[i]),
            pltpu.make_async_remote_copy(
                src_ref=src.at[:, :, theirs], dst_ref=dst.at[:, planes],
                send_sem=out_send.at[i], recv_sem=out_recv.at[i],
                device_id=(slab, other), device_id_type=MESH,
            ),
        )

    def results():
        return [deliver(e, ss.at[e], os_.at[e]) for e in range(ITERS)] + [
            deliver(ITERS + e, vv.at[e], ob.at[e + 1]) for e in range(ITERS - 1)
        ] + [deliver(2 * ITERS - 1, wl, ob.at[ITERS])]

    outs = results()

    def hand_over(i):
        for item in outs[i]:
            item.start()

    def turn(f):
        return (
            pltpu.roll(f, rows - 1, 0), pltpu.roll(f, 1, 0),
            pltpu.roll(f, nz - 1, 1), pltpu.roll(f, 1, 1),
        )

    def masked(f):
        yp, ym, zp, zm = turn(f)
        return yp * mk[0], ym * mk[1], zp * mk[2], zm * mk[3]

    def off_diagonal(below, around, above, k):
        yp, ym, zp, zm = around
        total = co[0, k] * above + co[1, k] * below
        total = total + (co[2, k] * yp + co[3, k] * ym)
        return total + (co[4, k] * zp + co[5, k] * zm)

    def inside(k):
        at = me * h + k
        return jnp.where(jnp.logical_and(at >= 0, at < n * h), 1.0, 0.0)

    def coefficients(k, carry):
        hx, hy, hz = 0.5 * raw[0, k], 0.5 * raw[1, k], 0.5 * raw[2, k]
        co[0, k] = 1.0 - hx
        co[1, k] = 1.0 + hx
        co[2, k] = (1.0 - hy) * mk[0]
        co[3, k] = (1.0 + hy) * mk[1]
        co[4, k] = (1.0 - hz) * mk[2]
        co[5, k] = (1.0 + hz) * mk[3]
        diagonal = 6.0 + raw[3, k]
        co[6, k] = diagonal
        co[7, k] = inside(k - 1) / diagonal
        return carry

    def masses(k, carry):
        co[8, k] = 1.0 / raw[4, k]
        return carry

    def guess(e):
        def body(k, carry):
            here = xp[e, k + 1]
            yp, ym, zp, zm = masked(here)
            total = (xp[e, k] + xp[e, k + 2]) + (yp + ym) + (zp + zm)
            t1[k] = (here + total * (1.0 / 7.0)) * (inside(k - 1) * (1.0 / 7.0))
            return carry
        return body

    def schur(e):
        def body(k, carry):
            here = t1[k + 1]
            off = off_diagonal(t1[k], turn(here), t1[k + 2], k + 1)
            qs[e, k + 2] = (off - co[6, k + 1] * here) * co[8, k + 1]
            return carry
        return body

    def velocity_first(e):
        def body(k, carry):
            yp, ym, zp, zm = masked(qs[e, k + 2])
            scale = co[7, k + 1]
            y0[e, 0, k + 2] = (xu[e, 0, k + 1] - 0.5 * (qs[e, k + 3] - qs[e, k + 1])) * scale
            y0[e, 1, k + 2] = (xu[e, 1, k + 1] - 0.5 * (yp - ym)) * scale
            y0[e, 2, k + 2] = (xu[e, 2, k + 1] - 0.5 * (zp - zm)) * scale
            return carry
        return body

    def velocity_second(e):
        def body(k, carry):
            for c in range(3):
                here = y0[e, c, k + 2]
                off = off_diagonal(y0[e, c, k + 1], turn(here), y0[e, c, k + 3], k + 1)
                z1[c, k + 1] = off * co[7, k + 1]
            return carry
        return body

    def image(e, factor, weights):
        def mix(value, held):
            if e > 0:
                value = value * factor
                for g, item in zip(weights, held):
                    value = value - g * item
            return value

        def body(k, carry):
            q = qs[e, k + 2]
            qa, qb = qs[e, k + 3], qs[e, k + 1]
            yp, ym, zp, zm = masked(q)
            low = 0.5 * ((qa + qb) + (yp + ym) + (zp + zm)) - 3.0 * q
            for c in range(3):
                here = z1[c, k + 1]
                off = off_diagonal(z1[c, k], turn(here), z1[c, k + 2], k + 1)
                value = mix(xu[e, c, k + 1] - off, [xu[i + 1, c, k + 1] for i in range(e)])
                full = y0[e, c, k + 2] + here
                if c == 0:
                    above = y0[e, 0, k + 3] + z1[0, k + 2]
                    below = y0[e, 0, k + 1] + z1[0, k]
                    low = low - 0.5 * (above - below)
                elif c == 1:
                    a, b = pltpu.roll(full, rows - 1, 0), pltpu.roll(full, 1, 0)
                    low = low - 0.5 * (a * mk[0] - b * mk[1])
                else:
                    a, b = pltpu.roll(full, nz - 1, 1), pltpu.roll(full, 1, 1)
                    low = low - 0.5 * (a * mk[2] - b * mk[3])
                ss[e, c, k] = mix(full, [ss[i, c, k] for i in range(e)])
                if e + 1 < ITERS:
                    xu[e + 1, c, k + 1] = value
                else:
                    wl[c, k] = value
            ss[e, 3, k] = mix(q, [ss[i, 3, k] for i in range(e)])
            value = mix(low, [xp[i + 1, k + 2] for i in range(e)])
            if e + 1 < ITERS:
                xp[e + 1, k + 2] = value
            else:
                wl[3, k] = value
            return carry
        return body

    def held_of(i, c, k):
        if i > 0:
            return vv[i - 1, c, k]
        return xp[0, k + 2] if c == 3 else xu[0, c, k + 1]

    def image_of(e, c, k):
        if e + 1 == ITERS:
            return wl[c, k]
        return xp[e + 1, k + 2] if c == 3 else xu[e + 1, c, k + 1]

    stages[0].wait()
    pl.semaphore_wait(barrier, n - 1)
    first_begin(0)
    first_copy(0, 0).start()
    for item in stages[1:4]:
        item.wait()
    first_begin(1)
    first_copy(1, 0).start()
    first_copy(2, 0).start()
    stages[4].wait()
    first_begin(3)
    first_copy(3, 0).start()
    for item in own[1:4]:
        item.wait()
    first_near(1)
    first_near(2)
    loop(h, coefficients, low=1)
    loop(h, masses, low=1)
    own[0].wait()
    first_near(0)
    first_far(0)

    zero = jnp.zeros((rows, nz), f32)
    inverses, entries = [], {}
    factor, weights = None, []
    for e in range(ITERS):
        if e > 0:
            arrive(0, e)
        loop(h + 2, guess(e))
        loop(h, schur(e))
        begin(2, e)
        if e == 0:
            own[4].wait()
            first_near(3)
        loop(h - 2, velocity_first(e), low=1)
        begin(3, e)
        if e == 0:
            first_far(1)
            coefficients(0, 0)
            coefficients(h + 1, 0)
            first_far(3)
        else:
            sums = reduce_end(e - 1, e + 1)
            norm = jnp.sqrt(sums[0])
            factor = 1.0 / norm
            if e > 1:
                entries[(e - 1, e - 2)] = norm
            inverses.append(factor)
            weights = []
            for i in range(e):
                value = sums[i + 1] * inverses[i] * factor
                entries[(i, e - 1)] = value
                weights.append(value * inverses[i])

            def form(k, carry, e=e):
                for c in range(4):
                    value = image_of(e - 1, c, k) * factor
                    for i in range(e):
                        value = value - weights[i] * held_of(i, c, k)
                    vv[e - 1, c, k] = value
                return carry

            loop(h, form)
            hand_over(ITERS + e - 1)
            arrive(1, e)
        arrive(2, e)
        for k in (0, h - 1, -1, h):
            velocity_first(e)(k, 0)
        loop(h, velocity_second(e))
        for c in range(3):
            z1[c, 0] = zero
            z1[c, h + 1] = zero
        loop(h, image(e, factor, weights))
        hand_over(e)
        arrive(3, e)

        scale = factor if e > 0 else 1.0

        def patch(c, e=e, scale=scale):
            low, high = [], []
            for k, found in ((-1, low), (h, high)):
                here = y0[e, c, k + 2]
                off = off_diagonal(y0[e, c, k + 1], turn(here), y0[e, c, k + 3], k + 1)
                found.append(off * co[7, k + 1] * scale)
            low, high = low[0], high[0]
            if e + 1 < ITERS:
                if c == 0:
                    xp[e + 1, 2] = xp[e + 1, 2] + 0.5 * low
                    xp[e + 1, h + 1] = xp[e + 1, h + 1] - 0.5 * high
                xu[e + 1, c, 1] = xu[e + 1, c, 1] - co[1, 1] * low
                xu[e + 1, c, h] = xu[e + 1, c, h] - co[0, h] * high
            else:
                if c == 0:
                    wl[3, 0] = wl[3, 0] + 0.5 * low
                    wl[3, h - 1] = wl[3, h - 1] - 0.5 * high
                wl[c, 0] = wl[c, 0] - co[1, 1] * low
                wl[c, h - 1] = wl[c, h - 1] - co[0, h] * high

        patch(0)
        if e + 1 < ITERS:
            begin(0, e + 1)
        patch(1)
        patch(2)
        if e + 1 == ITERS:
            hand_over(2 * ITERS - 1)

        def totals(k, acc, e=e):
            acc = list(acc)
            found = [image_of(e, c, k) for c in range(4)]
            for i in range(e + 1):
                held = [held_of(i, c, k) for c in range(4)]
                term = held[0] * found[0] + held[1] * found[1]
                acc[i + 1] = acc[i + 1] + (term + (held[2] * found[2] + held[3] * found[3]))
                if i == e:
                    term = held[0] * held[0] + held[1] * held[1]
                    acc[0] = acc[0] + (term + (held[2] * held[2] + held[3] * held[3]))
            if e + 1 == ITERS:
                term = found[0] * found[0] + found[1] * found[1]
                acc[e + 2] = acc[e + 2] + (term + (found[2] * found[2] + found[3] * found[3]))
            return tuple(acc)

        count = e + 2 if e + 1 < ITERS else e + 3
        reduce_start(e, loop(h, totals, (zero,) * count))
        if e + 1 < ITERS:
            begin(1, e + 1)

    for g in range(len(first)):
        first_finish(g)
    first_out.wait()
    for e in range(ITERS):
        for kind in range(4):
            if e > 0 or kind > 1:
                finish(kind, e)
    for here, there in outs:
        here.wait()
        there.wait()
    for e in range(ITERS - 1):
        red_wait(e, red_send)
    sums = reduce_end(ITERS - 1, ITERS + 2)
    norm = jnp.sqrt(sums[0])
    factor = 1.0 / norm
    entries[(ITERS - 1, ITERS - 2)] = norm
    inverses.append(factor)
    left = sums[ITERS + 1] * factor * factor
    spread = []
    for i in range(ITERS):
        value = sums[i + 1] * inverses[i] * factor
        entries[(i, ITERS - 1)] = value
        spread.append(value * inverses[i])
        left = left - value * value
    norm = jnp.sqrt(left)
    entries[(ITERS, ITERS - 1)] = norm
    inverse = 1.0 / norm
    lines = inverses + [factor * inverse] + [g * inverse for g in spread]
    for i, value in enumerate(lines):
        scal[i : i + 1] = jnp.broadcast_to(value, (1, LANES))
    r = lax.broadcasted_iota(jnp.int32, (8, LANES), 0)
    c = lax.broadcasted_iota(jnp.int32, (8, LANES), 1)
    table = jnp.zeros((8, LANES), f32)
    for (i, j), value in entries.items():
        table = table + jnp.where(jnp.logical_and(r == i, c == j), value, 0.0)
    scal[8:16] = table
    red_wait(ITERS - 1, red_send)


def write(ob, os_, scal, basis, search, hess, bb, sb, hb, sems):
    def value(i):
        return scal[i : i + 1, 0:1]

    copies = []

    def emit(src, dst, i):
        item = pltpu.make_async_copy(src, dst, sems.at[i])
        item.start()
        copies.append(item)

    hb[...] = scal[8 : 8 + ITERS + 1, 0:ITERS]
    emit(hb, hess, 2 * ITERS + 1)
    planes = ob.shape[2]
    inverse = [value(i) for i in range(ITERS)]
    for e in range(ITERS):
        def body(k, carry, e=e):
            for c in range(4):
                bb[e, c, k] = ob[e, c, k] * inverse[e]
                sb[e, c, k] = os_[e, c, k] * inverse[e]
            return carry

        loop(planes, body)
        emit(bb.at[e], basis.at[e], e)
        emit(sb.at[e], search.at[e], ITERS + 1 + e)
    weights = [value(ITERS + i) for i in range(ITERS + 1)]

    def last(k, carry):
        for c in range(4):
            total = ob[ITERS, c, k] * weights[0]
            for i in range(ITERS):
                total = total - weights[i + 1] * ob[i, c, k]
            bb[ITERS, c, k] = total
        return carry

    loop(planes, last)
    emit(bb.at[ITERS], basis.at[ITERS], ITERS)
    for item in copies:
        item.wait()


def per_device(slabs, subs, start, wind, reaction, mass):
    _, cx, cy, nz = start.shape
    n = slabs * subs
    rows, h = subs * cy, cx // subs
    assert subs == 2 and cx % subs == 0 and h >= 3
    f32 = jnp.float32

    def field(*lead):
        return pltpu.VMEM((*lead, rows, nz), f32)

    anywhere = pl.BlockSpec(memory_space=pl.ANY)
    vmem = pl.BlockSpec(memory_space=pltpu.VMEM)
    hbm = pl.BlockSpec(memory_space=pltpu.HBM)
    ob, os_, scal = pl.pallas_call(
        functools.partial(kernel, slabs, subs, cx, cy, nz),
        out_shape=(
            jax.ShapeDtypeStruct((ITERS + 1, 4, cx, cy, nz), f32),
            jax.ShapeDtypeStruct((ITERS, 4, cx, cy, nz), f32),
            jax.ShapeDtypeStruct((16, LANES), f32),
        ),
        in_specs=[hbm] * 4,
        out_specs=(anywhere, anywhere, vmem),
        scratch_shapes=[
            pltpu.VMEM((9, cx, cy, nz), f32),
            field(ITERS, h + 4),
            field(ITERS, 3, h + 2),
            field(ITERS, h + 4),
            field(ITERS, 3, h + 4),
            field(h + 2),
            field(3, h + 2),
            field(5, h + 2),
            field(9, h + 2),
            field(4),
            field(ITERS - 1, 4, h),
            field(ITERS, 4, h),
            field(4, h),
            pltpu.VMEM((ITERS, n, 1, LANES), f32),
            pltpu.SemaphoreType.DMA((4, 3)),
            pltpu.SemaphoreType.DMA((4, 3)),
            pltpu.SemaphoreType.DMA((4, ITERS, 2)),
            pltpu.SemaphoreType.DMA((4, ITERS, 2)),
            pltpu.SemaphoreType.DMA((ITERS,)),
            pltpu.SemaphoreType.DMA((ITERS,)),
            pltpu.SemaphoreType.DMA((11,)),
            pltpu.SemaphoreType.DMA((2 * ITERS,)),
            pltpu.SemaphoreType.DMA((2 * ITERS,)),
            pltpu.SemaphoreType.DMA((2 * ITERS,)),
        ],
        compiler_params=pltpu.CompilerParams(
            collective_id=0, has_side_effects=True, vmem_limit_bytes=40_000_000
        ),
    )(start, wind, reaction, mass)
    return pl.pallas_call(
        write,
        out_shape=(
            jax.ShapeDtypeStruct((ITERS + 1, 4, cx, cy, nz), f32),
            jax.ShapeDtypeStruct((ITERS, 4, cx, cy, nz), f32),
            jax.ShapeDtypeStruct((ITERS + 1, ITERS), f32),
        ),
        in_specs=[vmem] * 3,
        out_specs=(hbm, hbm, hbm),
        scratch_shapes=[
            pltpu.VMEM((ITERS + 1, 4, cx, cy, nz), f32),
            pltpu.VMEM((ITERS, 4, cx, cy, nz), f32),
            pltpu.VMEM((ITERS + 1, ITERS), f32),
            pltpu.SemaphoreType.DMA((2 * ITERS + 2,)),
        ],
        compiler_params=pltpu.CompilerParams(vmem_limit_bytes=10_000_000),
    )(ob, os_, scal)


def solution(mesh):
    slabs, subs = mesh.shape["slab"], mesh.shape["sub"]
    return jax.shard_map(
        functools.partial(per_device, slabs, subs),
        mesh=mesh,
        in_specs=(
            P(None, "slab", "sub", None),
            P(None, "slab", "sub", None),
            P("slab", "sub", None),
            P("slab", "sub", None),
        ),
        out_specs=(P(None, None, "slab", "sub", None), P(None, None, "slab", "sub", None), P()),
        check_vma=False,
    )
```

```python
import functools

import jax
import jax.numpy as jnp
from jax import lax
from jax.experimental import pallas as pl
from jax.experimental.pallas import tpu as pltpu
from jax.sharding import PartitionSpec as P

ITERS = 3
UNROLL = 5
LANES = 128
MESH = pl.DeviceIdType.MESH


def fold(x):
    rows, cols = x.shape
    total = None
    for r in range(0, rows, 8):
        for c in range(0, cols, LANES):
            piece = x[r : r + 8, c : c + LANES]
            total = piece if total is None else total + piece
    return total


def loop(count, body, init=0, low=0):
    step = max(u for u in range(1, UNROLL + 1) if count % u == 0)

    def several(k, carry):
        for i in range(step):
            carry = body(low + k * step + i, carry)
        return carry

    return lax.fori_loop(0, count // step, several, init)


def kernel(
    slabs, subs, cx, cy, nz,
    start, wind, reaction, mass, ob, os_, scal,
    stage, xp, xu, qs, y0, t1, z1, raw, co, mk, vv, ss, wl, red,
    init_send, init_recv, send, recv, red_send, red_recv, load, out_local, out_send, out_recv, known,
):
    slab, sub = lax.axis_index("slab"), lax.axis_index("sub")
    n = slabs * subs
    me = slab * subs + sub
    h = cx // subs
    rows = subs * cy
    f32 = jnp.float32
    other = 1 - sub
    has_left, has_right = me > 0, me < n - 1
    has_cross = jnp.where(sub == 0, slab, slabs - 1 - slab) > 0
    mine = pl.ds(pl.multiple_of(sub * cy, 8), cy)
    theirs = pl.ds(pl.multiple_of(other * cy, 8), cy)

    def staged(lo, count):
        return lambda planes: stage.at[pl.ds(lo, count), planes]

    first = [
        (lambda planes: stage.at[3, planes], lambda planes, lines: xp.at[0, planes, lines], 2, 2),
        (staged(4, 4), lambda planes, lines: raw.at[pl.ds(0, 4), planes, lines], 1, 1),
        (lambda planes: stage.at[8, planes], lambda planes, lines: raw.at[4, planes, lines], 1, 0),
        (staged(0, 3), lambda planes, lines: xu.at[0, :, planes, lines], 1, 1),
    ]

    def window(g, side):
        _, _, at, w = first[g]
        return pl.ds(side * (h - w), h + w), pl.ds(at - side * w, h + w)

    def local(g, src, dst, sem):
        a, b = window(g, sub)
        return pltpu.make_async_copy(src(a), dst(b), load.at[sem])

    stages = [
        pltpu.make_async_copy(start.at[3], stage.at[3], load.at[0]),
        pltpu.make_async_copy(wind, stage.at[pl.ds(4, 3)], load.at[1]),
        pltpu.make_async_copy(reaction, stage.at[7], load.at[2]),
        pltpu.make_async_copy(mass, stage.at[8], load.at[3]),
        pltpu.make_async_copy(start.at[pl.ds(0, 3)], stage.at[pl.ds(0, 3)], load.at[4]),
    ]
    own = [
        local(0, lambda a: start.at[3, a], lambda b: xp.at[0, b, mine], 5),
        local(1, lambda a: wind.at[:, a], lambda b: raw.at[pl.ds(0, 3), b, mine], 6),
        local(1, lambda a: reaction.at[a], lambda b: raw.at[3, b, mine], 7),
        local(2, lambda a: mass.at[a], lambda b: raw.at[4, b, mine], 8),
        local(3, lambda a: start.at[pl.ds(0, 3), a], lambda b: xu.at[0, :, b, mine], 9),
    ]
    first_out = pltpu.make_async_copy(start, ob.at[0], load.at[10])
    for item in stages:
        item.start()
    for item in own:
        item.start()
    first_out.start()

    barrier = pltpu.get_barrier_semaphore()

    def greet(sem, at, core):
        pl.semaphore_signal(sem, inc=1, device_id=(at, core), device_id_type=MESH)

    def near(way):
        for core in range(subs):
            greet(barrier, slab + way, core)

    greet(barrier, slab, other)
    pl.when(slab > 0)(lambda: near(-1))
    pl.when(slab < slabs - 1)(lambda: near(1))
    met = 1 + jnp.where(slab > 0, subs, 0) + jnp.where(slab < slabs - 1, subs, 0)
    steps = [1 << i for i in range((slabs - 1).bit_length())]

    def spread(i):
        d = steps[i]
        pl.when(slab + d < slabs)(lambda: greet(known.at[i, 0], slab + d, sub))
        pl.when(slab - d >= 0)(lambda: greet(known.at[i, 1], slab - d, sub))

    def gather(i):
        d = steps[i]
        pl.when(slab - d >= 0)(lambda: pl.semaphore_wait(known.at[i, 0], 1))
        pl.when(slab + d < slabs)(lambda: pl.semaphore_wait(known.at[i, 1], 1))

    def further(count):
        for _ in range(count):
            if pending:
                i = pending.pop(0)
                gather(i)
                if i + 1 < len(steps):
                    spread(i + 1)

    pending = list(range(len(steps)))

    def clear(low):
        def inner():
            zero = jnp.zeros((rows, nz), f32)
            for e in range(ITERS):
                for k in range(2):
                    at = k if low else 2 + h + k
                    xp[e, at] = zero
                    qs[e, at] = zero
                for c in range(3):
                    xu[e, c, 0 if low else 1 + h] = zero
                    y0[e, c, 0 if low else 3 + h] = zero
            for c in range(4):
                raw[c, 0 if low else 1 + h] = zero
        return inner

    pl.when(jnp.logical_not(has_left))(clear(True))
    pl.when(jnp.logical_not(has_right))(clear(False))

    row = lax.broadcasted_iota(jnp.int32, (rows, nz), 0)
    col = lax.broadcasted_iota(jnp.int32, (rows, nz), 1)
    mk[0] = jnp.where(row == rows - 1, 0.0, 1.0)
    mk[1] = jnp.where(row == 0, 0.0, 1.0)
    mk[2] = jnp.where(col == nz - 1, 0.0, 1.0)
    mk[3] = jnp.where(col == 0, 0.0, 1.0)

    def first_copy(g, kind):
        src, dst, at, w = first[g]
        if kind == 0:
            a, b = window(g, other)
            target, slot = (slab, other), 0
        elif kind == 1:
            a, b = pl.ds(cx - w, w), pl.ds(at - w, w)
            target, slot = (slab + 1, 0), 1 + sub
        else:
            a, b = pl.ds(0, w), pl.ds(at + h, w)
            target, slot = (slab - 1, subs - 1), 1 + sub
        return pltpu.make_async_remote_copy(
            src_ref=src(a), dst_ref=dst(b, mine), send_sem=init_send.at[g, kind],
            recv_sem=init_recv.at[g, slot], device_id=target, device_id_type=MESH,
        )

    def first_begin(g):
        if first[g][3] > 0:
            pl.when(slab < slabs - 1)(lambda: first_copy(g, 1).start())
            pl.when(slab > 0)(lambda: first_copy(g, 2).start())

    def first_wait(ref, sem):
        pltpu.make_async_copy(ref, ref, sem).wait()

    def first_near(g):
        _, dst, _, _ = first[g]
        _, b = window(g, sub)
        first_wait(dst(b, theirs), init_recv.at[g, 0])

    def first_far(g):
        _, dst, at, w = first[g]
        if w > 0:
            def inner():
                for r in range(subs):
                    first_wait(dst(pl.ds(0, w), pl.ds(r * cy, cy)), init_recv.at[g, 1 + r])
            pl.when(has_cross)(inner)

    def first_finish(g):
        first_copy(g, 0).wait_send()
        if first[g][3] > 0:
            pl.when(slab < slabs - 1)(lambda: first_copy(g, 1).wait_send())
            pl.when(slab > 0)(lambda: first_copy(g, 2).wait_send())

    def remote(kind, e, way):
        if kind == 0 or kind == 2:
            ref = (xp, None, qs)[kind].at[e]
            pair = (pl.ds(h, 2), pl.ds(0, 2)) if way == 0 else (pl.ds(2, 2), pl.ds(h + 2, 2))
            src, dst = ref.at[pair[0]], ref.at[pair[1]]
        elif kind == 1:
            pair = (h, 0) if way == 0 else (1, h + 1)
            src, dst = xu.at[e, :, pair[0]], xu.at[e, :, pair[1]]
        else:
            pair = (h, 0) if way == 0 else (3, h + 3)
            src, dst = y0.at[e, :, pair[0]], y0.at[e, :, pair[1]]
        target = me + 1 if way == 0 else me - 1
        return pltpu.make_async_remote_copy(
            src_ref=src, dst_ref=dst, send_sem=send.at[kind, e, way], recv_sem=recv.at[kind, e, way],
            device_id=(target // subs, lax.rem(target, subs)), device_id_type=MESH,
        )

    def begin(kind, e):
        pl.when(has_right)(lambda: remote(kind, e, 0).start())
        pl.when(has_left)(lambda: remote(kind, e, 1).start())

    def arrive(kind, e):
        pl.when(has_left)(lambda: remote(kind, e, 0).wait_recv())
        pl.when(has_right)(lambda: remote(kind, e, 1).wait_recv())

    def finish(kind, e):
        pl.when(has_right)(lambda: remote(kind, e, 0).wait_send())
        pl.when(has_left)(lambda: remote(kind, e, 1).wait_send())

    lane = lax.broadcasted_iota(jnp.int32, (1, LANES), 1)

    def reduce_start(e, parts):
        line = jnp.zeros((1, LANES), f32)
        for i, part in enumerate(parts):
            line = line + jnp.where(lane == i, jnp.sum(fold(part), keepdims=True), 0.0)
        red[e, me] = line

        def tell(at, core):
            pltpu.make_async_remote_copy(
                src_ref=red.at[e, me], dst_ref=red.at[e, me],
                send_sem=red_send.at[e], recv_sem=red_recv.at[e],
                device_id=(at, core), device_id_type=MESH,
            ).start()

        def push(k, carry):
            at = lax.rem(slab + k, slabs)
            for core in range(subs):
                tell(at, core)
            return carry

        lax.fori_loop(1, slabs, push, 0)
        tell(slab, other)

    def red_wait(e, sem):
        block = red.at[e, pl.ds(0, n - 1)]
        pltpu.make_async_copy(block, block, sem.at[e]).wait()

    def reduce_end(e, count):
        red_wait(e, red_recv)
        total = jnp.sum(red[e], axis=0)
        return [
            jnp.sum(jnp.where(lane == i, total, 0.0), axis=1, keepdims=True)
            for i in range(count)
        ]

    def deliver(i, src, dst):
        planes = pl.ds(sub * h, h)
        return (
            pltpu.make_async_copy(src.at[:, :, mine], dst.at[:, planes], out_local.at[i]),
            pltpu.make_async_remote_copy(
                src_ref=src.at[:, :, theirs], dst_ref=dst.at[:, planes],
                send_sem=out_send.at[i], recv_sem=out_recv.at[i],
                device_id=(slab, other), device_id_type=MESH,
            ),
        )

    def results():
        return [deliver(e, ss.at[e], os_.at[e]) for e in range(ITERS)] + [
            deliver(ITERS + e, vv.at[e], ob.at[e + 1]) for e in range(ITERS - 1)
        ] + [deliver(2 * ITERS - 1, wl, ob.at[ITERS])]

    outs = results()

    def hand_over(i):
        for item in outs[i]:
            item.start()

    def turn(f):
        return (
            pltpu.roll(f, rows - 1, 0), pltpu.roll(f, 1, 0),
            pltpu.roll(f, nz - 1, 1), pltpu.roll(f, 1, 1),
        )

    def masked(f):
        yp, ym, zp, zm = turn(f)
        return yp * mk[0], ym * mk[1], zp * mk[2], zm * mk[3]

    def off_diagonal(below, around, above, k):
        yp, ym, zp, zm = around
        total = co[0, k] * above + co[1, k] * below
        total = total + (co[2, k] * yp + co[3, k] * ym)
        return total + (co[4, k] * zp + co[5, k] * zm)

    def inside(k):
        at = me * h + k
        return jnp.where(jnp.logical_and(at >= 0, at < n * h), 1.0, 0.0)

    def coefficients(k, carry):
        hx, hy, hz = 0.5 * raw[0, k], 0.5 * raw[1, k], 0.5 * raw[2, k]
        co[0, k] = 1.0 - hx
        co[1, k] = 1.0 + hx
        co[2, k] = (1.0 - hy) * mk[0]
        co[3, k] = (1.0 + hy) * mk[1]
        co[4, k] = (1.0 - hz) * mk[2]
        co[5, k] = (1.0 + hz) * mk[3]
        diagonal = 6.0 + raw[3, k]
        co[6, k] = diagonal
        co[7, k] = inside(k - 1) / diagonal
        return carry

    def masses(k, carry):
        co[8, k] = 1.0 / raw[4, k]
        return carry

    def guess(e):
        def body(k, carry):
            here = xp[e, k + 1]
            yp, ym, zp, zm = masked(here)
            total = (xp[e, k] + xp[e, k + 2]) + (yp + ym) + (zp + zm)
            t1[k] = (here + total * (1.0 / 7.0)) * (inside(k - 1) * (1.0 / 7.0))
            return carry
        return body

    def schur(e):
        def body(k, carry):
            here = t1[k + 1]
            off = off_diagonal(t1[k], turn(here), t1[k + 2], k + 1)
            qs[e, k + 2] = (off - co[6, k + 1] * here) * co[8, k + 1]
            return carry
        return body

    def velocity_first(e):
        def body(k, carry):
            yp, ym, zp, zm = masked(qs[e, k + 2])
            scale = co[7, k + 1]
            y0[e, 0, k + 2] = (xu[e, 0, k + 1] - 0.5 * (qs[e, k + 3] - qs[e, k + 1])) * scale
            y0[e, 1, k + 2] = (xu[e, 1, k + 1] - 0.5 * (yp - ym)) * scale
            y0[e, 2, k + 2] = (xu[e, 2, k + 1] - 0.5 * (zp - zm)) * scale
            return carry
        return body

    def velocity_second(e):
        def body(k, carry):
            for c in range(3):
                here = y0[e, c, k + 2]
                off = off_diagonal(y0[e, c, k + 1], turn(here), y0[e, c, k + 3], k + 1)
                z1[c, k + 1] = off * co[7, k + 1]
            return carry
        return body

    def image(e, factor, weights):
        def mix(value, held):
            if e > 0:
                value = value * factor
                for g, item in zip(weights, held):
                    value = value - g * item
            return value

        def body(k, carry):
            q = qs[e, k + 2]
            qa, qb = qs[e, k + 3], qs[e, k + 1]
            yp, ym, zp, zm = masked(q)
            low = 0.5 * ((qa + qb) + (yp + ym) + (zp + zm)) - 3.0 * q
            for c in range(3):
                here = z1[c, k + 1]
                off = off_diagonal(z1[c, k], turn(here), z1[c, k + 2], k + 1)
                value = mix(xu[e, c, k + 1] - off, [xu[i + 1, c, k + 1] for i in range(e)])
                full = y0[e, c, k + 2] + here
                if c == 0:
                    above = y0[e, 0, k + 3] + z1[0, k + 2]
                    below = y0[e, 0, k + 1] + z1[0, k]
                    low = low - 0.5 * (above - below)
                elif c == 1:
                    a, b = pltpu.roll(full, rows - 1, 0), pltpu.roll(full, 1, 0)
                    low = low - 0.5 * (a * mk[0] - b * mk[1])
                else:
                    a, b = pltpu.roll(full, nz - 1, 1), pltpu.roll(full, 1, 1)
                    low = low - 0.5 * (a * mk[2] - b * mk[3])
                ss[e, c, k] = mix(full, [ss[i, c, k] for i in range(e)])
                if e + 1 < ITERS:
                    xu[e + 1, c, k + 1] = value
                else:
                    wl[c, k] = value
            ss[e, 3, k] = mix(q, [ss[i, 3, k] for i in range(e)])
            value = mix(low, [xp[i + 1, k + 2] for i in range(e)])
            if e + 1 < ITERS:
                xp[e + 1, k + 2] = value
            else:
                wl[3, k] = value
            return carry
        return body

    def held_of(i, c, k):
        if i > 0:
            return vv[i - 1, c, k]
        return xp[0, k + 2] if c == 3 else xu[0, c, k + 1]

    def image_of(e, c, k):
        if e + 1 == ITERS:
            return wl[c, k]
        return xp[e + 1, k + 2] if c == 3 else xu[e + 1, c, k + 1]

    stages[0].wait()
    pl.semaphore_wait(barrier, met)
    first_begin(0)
    first_copy(0, 0).start()
    spread(0)
    for item in stages[1:4]:
        item.wait()
    first_begin(1)
    first_copy(1, 0).start()
    first_copy(2, 0).start()
    stages[4].wait()
    first_begin(3)
    first_copy(3, 0).start()
    for item in own[1:4]:
        item.wait()
    first_near(1)
    first_near(2)
    loop(h, coefficients, low=1)
    loop(h, masses, low=1)
    further(1)
    own[0].wait()
    first_near(0)
    first_far(0)

    zero = jnp.zeros((rows, nz), f32)
    inverses, entries = [], {}
    factor, weights = None, []
    for e in range(ITERS):
        if e > 0:
            arrive(0, e)
        loop(h + 2, guess(e))
        loop(h, schur(e))
        begin(2, e)
        if e == 0:
            further(1)
            own[4].wait()
            first_near(3)
        loop(h - 2, velocity_first(e), low=1)
        begin(3, e)
        if e == 0:
            first_far(1)
            coefficients(0, 0)
            coefficients(h + 1, 0)
            first_far(3)
            further(1)
        else:
            sums = reduce_end(e - 1, e + 1)
            norm = jnp.sqrt(sums[0])
            factor = 1.0 / norm
            if e > 1:
                entries[(e - 1, e - 2)] = norm
            inverses.append(factor)
            weights = []
            for i in range(e):
                value = sums[i + 1] * inverses[i] * factor
                entries[(i, e - 1)] = value
                weights.append(value * inverses[i])

            def form(k, carry, e=e):
                for c in range(4):
                    value = image_of(e - 1, c, k) * factor
                    for i in range(e):
                        value = value - weights[i] * held_of(i, c, k)
                    vv[e - 1, c, k] = value
                return carry

            loop(h, form)
            hand_over(ITERS + e - 1)
            arrive(1, e)
        arrive(2, e)
        for k in (0, h - 1, -1, h):
            velocity_first(e)(k, 0)
        loop(h, velocity_second(e))
        for c in range(3):
            z1[c, 0] = zero
            z1[c, h + 1] = zero
        loop(h, image(e, factor, weights))
        hand_over(e)
        if e == 0:
            further(len(steps))
        arrive(3, e)

        scale = factor if e > 0 else 1.0

        def patch(c, e=e, scale=scale):
            low, high = [], []
            for k, found in ((-1, low), (h, high)):
                here = y0[e, c, k + 2]
                off = off_diagonal(y0[e, c, k + 1], turn(here), y0[e, c, k + 3], k + 1)
                found.append(off * co[7, k + 1] * scale)
            low, high = low[0], high[0]
            if e + 1 < ITERS:
                if c == 0:
                    xp[e + 1, 2] = xp[e + 1, 2] + 0.5 * low
                    xp[e + 1, h + 1] = xp[e + 1, h + 1] - 0.5 * high
                xu[e + 1, c, 1] = xu[e + 1, c, 1] - co[1, 1] * low
                xu[e + 1, c, h] = xu[e + 1, c, h] - co[0, h] * high
            else:
                if c == 0:
                    wl[3, 0] = wl[3, 0] + 0.5 * low
                    wl[3, h - 1] = wl[3, h - 1] - 0.5 * high
                wl[c, 0] = wl[c, 0] - co[1, 1] * low
                wl[c, h - 1] = wl[c, h - 1] - co[0, h] * high

        patch(0)
        if e + 1 < ITERS:
            begin(0, e + 1)
        patch(1)
        patch(2)
        if e + 1 == ITERS:
            hand_over(2 * ITERS - 1)

        def totals(k, acc, e=e):
            acc = list(acc)
            found = [image_of(e, c, k) for c in range(4)]
            for i in range(e + 1):
                held = [held_of(i, c, k) for c in range(4)]
                term = held[0] * found[0] + held[1] * found[1]
                acc[i + 1] = acc[i + 1] + (term + (held[2] * found[2] + held[3] * found[3]))
                if i == e:
                    term = held[0] * held[0] + held[1] * held[1]
                    acc[0] = acc[0] + (term + (held[2] * held[2] + held[3] * held[3]))
            if e + 1 == ITERS:
                term = found[0] * found[0] + found[1] * found[1]
                acc[e + 2] = acc[e + 2] + (term + (found[2] * found[2] + found[3] * found[3]))
            return tuple(acc)

        count = e + 2 if e + 1 < ITERS else e + 3
        reduce_start(e, loop(h, totals, (zero,) * count))
        if e + 1 < ITERS:
            begin(1, e + 1)

    for g in range(len(first)):
        first_finish(g)
    first_out.wait()
    for e in range(ITERS):
        for kind in range(4):
            if e > 0 or kind > 1:
                finish(kind, e)
    for here, there in outs:
        here.wait()
        there.wait()
    for e in range(ITERS - 1):
        red_wait(e, red_send)
    sums = reduce_end(ITERS - 1, ITERS + 2)
    norm = jnp.sqrt(sums[0])
    factor = 1.0 / norm
    entries[(ITERS - 1, ITERS - 2)] = norm
    inverses.append(factor)
    left = sums[ITERS + 1] * factor * factor
    spread = []
    for i in range(ITERS):
        value = sums[i + 1] * inverses[i] * factor
        entries[(i, ITERS - 1)] = value
        spread.append(value * inverses[i])
        left = left - value * value
    norm = jnp.sqrt(left)
    entries[(ITERS, ITERS - 1)] = norm
    inverse = 1.0 / norm
    lines = inverses + [factor * inverse] + [g * inverse for g in spread]
    for i, value in enumerate(lines):
        scal[i : i + 1] = jnp.broadcast_to(value, (1, LANES))
    r = lax.broadcasted_iota(jnp.int32, (8, LANES), 0)
    c = lax.broadcasted_iota(jnp.int32, (8, LANES), 1)
    table = jnp.zeros((8, LANES), f32)
    for (i, j), value in entries.items():
        table = table + jnp.where(jnp.logical_and(r == i, c == j), value, 0.0)
    scal[8:16] = table
    red_wait(ITERS - 1, red_send)


def write(ob, os_, scal, basis, search, hess, bb, sb, hb, sems):
    def value(i):
        return scal[i : i + 1, 0:1]

    copies = []

    def emit(src, dst, i):
        item = pltpu.make_async_copy(src, dst, sems.at[i])
        item.start()
        copies.append(item)

    hb[...] = scal[8 : 8 + ITERS + 1, 0:ITERS]
    emit(hb, hess, 2 * ITERS + 1)
    planes = ob.shape[2]
    inverse = [value(i) for i in range(ITERS)]
    for e in range(ITERS):
        def body(k, carry, e=e):
            for c in range(4):
                bb[e, c, k] = ob[e, c, k] * inverse[e]
                sb[e, c, k] = os_[e, c, k] * inverse[e]
            return carry

        loop(planes, body)
        emit(bb.at[e], basis.at[e], e)
        emit(sb.at[e], search.at[e], ITERS + 1 + e)
    weights = [value(ITERS + i) for i in range(ITERS + 1)]

    def last(k, carry):
        for c in range(4):
            total = ob[ITERS, c, k] * weights[0]
            for i in range(ITERS):
                total = total - weights[i + 1] * ob[i, c, k]
            bb[ITERS, c, k] = total
        return carry

    loop(planes, last)
    emit(bb.at[ITERS], basis.at[ITERS], ITERS)
    for item in copies:
        item.wait()


def per_device(slabs, subs, start, wind, reaction, mass):
    _, cx, cy, nz = start.shape
    n = slabs * subs
    rows, h = subs * cy, cx // subs
    assert subs == 2 and cx % subs == 0 and h >= 3
    f32 = jnp.float32

    def field(*lead):
        return pltpu.VMEM((*lead, rows, nz), f32)

    anywhere = pl.BlockSpec(memory_space=pl.ANY)
    vmem = pl.BlockSpec(memory_space=pltpu.VMEM)
    hbm = pl.BlockSpec(memory_space=pltpu.HBM)
    ob, os_, scal = pl.pallas_call(
        functools.partial(kernel, slabs, subs, cx, cy, nz),
        out_shape=(
            jax.ShapeDtypeStruct((ITERS + 1, 4, cx, cy, nz), f32),
            jax.ShapeDtypeStruct((ITERS, 4, cx, cy, nz), f32),
            jax.ShapeDtypeStruct((16, LANES), f32),
        ),
        in_specs=[hbm] * 4,
        out_specs=(anywhere, anywhere, vmem),
        scratch_shapes=[
            pltpu.VMEM((9, cx, cy, nz), f32),
            field(ITERS, h + 4),
            field(ITERS, 3, h + 2),
            field(ITERS, h + 4),
            field(ITERS, 3, h + 4),
            field(h + 2),
            field(3, h + 2),
            field(5, h + 2),
            field(9, h + 2),
            field(4),
            field(ITERS - 1, 4, h),
            field(ITERS, 4, h),
            field(4, h),
            pltpu.VMEM((ITERS, n, 1, LANES), f32),
            pltpu.SemaphoreType.DMA((4, 3)),
            pltpu.SemaphoreType.DMA((4, 3)),
            pltpu.SemaphoreType.DMA((4, ITERS, 2)),
            pltpu.SemaphoreType.DMA((4, ITERS, 2)),
            pltpu.SemaphoreType.DMA((ITERS,)),
            pltpu.SemaphoreType.DMA((ITERS,)),
            pltpu.SemaphoreType.DMA((11,)),
            pltpu.SemaphoreType.DMA((2 * ITERS,)),
            pltpu.SemaphoreType.DMA((2 * ITERS,)),
            pltpu.SemaphoreType.DMA((2 * ITERS,)),
            pltpu.SemaphoreType.REGULAR(((slabs - 1).bit_length(), 2)),
        ],
        compiler_params=pltpu.CompilerParams(
            collective_id=0, has_side_effects=True, vmem_limit_bytes=40_000_000
        ),
    )(*(pltpu.with_memory_space_constraint(x, pltpu.HBM) for x in (start, wind, reaction, mass)))
    return pl.pallas_call(
        write,
        out_shape=(
            jax.ShapeDtypeStruct((ITERS + 1, 4, cx, cy, nz), f32),
            jax.ShapeDtypeStruct((ITERS, 4, cx, cy, nz), f32),
            jax.ShapeDtypeStruct((ITERS + 1, ITERS), f32),
        ),
        in_specs=[vmem] * 3,
        out_specs=(hbm, hbm, hbm),
        scratch_shapes=[
            pltpu.VMEM((ITERS + 1, 4, cx, cy, nz), f32),
            pltpu.VMEM((ITERS, 4, cx, cy, nz), f32),
            pltpu.VMEM((ITERS + 1, ITERS), f32),
            pltpu.SemaphoreType.DMA((2 * ITERS + 2,)),
        ],
        compiler_params=pltpu.CompilerParams(vmem_limit_bytes=10_000_000),
    )(ob, os_, scal)


def solution(mesh):
    slabs, subs = mesh.shape["slab"], mesh.shape["sub"]
    return jax.shard_map(
        functools.partial(per_device, slabs, subs),
        mesh=mesh,
        in_specs=(
            P(None, "slab", "sub", None),
            P(None, "slab", "sub", None),
            P("slab", "sub", None),
            P("slab", "sub", None),
        ),
        out_specs=(P(None, None, "slab", "sub", None), P(None, None, "slab", "sub", None), P()),
        check_vma=False,
    )
```

```python
import functools

import jax
import jax.numpy as jnp
from jax import lax
from jax.experimental import pallas as pl
from jax.experimental.pallas import tpu as pltpu
from jax.sharding import PartitionSpec as P

ITERS = 3
UNROLL = 5
LANES = 128
MESH = pl.DeviceIdType.MESH


def fold(x):
    rows, cols = x.shape
    total = None
    for r in range(0, rows, 8):
        for c in range(0, cols, LANES):
            piece = x[r : r + 8, c : c + LANES]
            total = piece if total is None else total + piece
    return total


def loop(count, body, init=0, low=0):
    step = max(u for u in range(1, UNROLL + 1) if count % u == 0)

    def several(k, carry):
        for i in range(step):
            carry = body(low + k * step + i, carry)
        return carry

    return lax.fori_loop(0, count // step, several, init)


def kernel(
    slabs, subs, cx, cy, nz,
    start, wind, reaction, mass, ob, os_, scal,
    stage, xp, xu, qs, y0, yq, t1, z1, raw, co, ca, mk, vv, ss, wl, red,
    init_send, init_recv, send, recv, red_send, red_recv, load, out_local, out_send, out_recv, known,
):
    slab, sub = lax.axis_index("slab"), lax.axis_index("sub")
    n = slabs * subs
    me = slab * subs + sub
    h = cx // subs
    rows = subs * cy
    f32 = jnp.float32
    other = 1 - sub
    has_left, has_right = me > 0, me < n - 1
    has_cross = jnp.where(sub == 0, slab, slabs - 1 - slab) > 0
    mine = pl.ds(pl.multiple_of(sub * cy, 8), cy)
    theirs = pl.ds(pl.multiple_of(other * cy, 8), cy)

    def staged(lo, count):
        return lambda planes: stage.at[pl.ds(lo, count), planes]

    first = [
        (lambda planes: stage.at[3, planes], lambda planes, lines: xp.at[0, planes, lines], 2, 2),
        (staged(4, 4), lambda planes, lines: raw.at[pl.ds(0, 4), planes, lines], 1, 1),
        (lambda planes: stage.at[8, planes], lambda planes, lines: raw.at[4, planes, lines], 1, 0),
        (staged(0, 3), lambda planes, lines: xu.at[0, :, planes, lines], 1, 1),
    ]

    def window(g, side):
        _, _, at, w = first[g]
        return pl.ds(side * (h - w), h + w), pl.ds(at - side * w, h + w)

    def local(g, src, dst, sem):
        a, b = window(g, sub)
        return pltpu.make_async_copy(src(a), dst(b), load.at[sem])

    stages = [
        pltpu.make_async_copy(start.at[3], stage.at[3], load.at[0]),
        pltpu.make_async_copy(wind, stage.at[pl.ds(4, 3)], load.at[1]),
        pltpu.make_async_copy(reaction, stage.at[7], load.at[2]),
        pltpu.make_async_copy(mass, stage.at[8], load.at[3]),
        pltpu.make_async_copy(start.at[pl.ds(0, 3)], stage.at[pl.ds(0, 3)], load.at[4]),
    ]
    own = [
        local(0, lambda a: start.at[3, a], lambda b: xp.at[0, b, mine], 5),
        local(1, lambda a: wind.at[:, a], lambda b: raw.at[pl.ds(0, 3), b, mine], 6),
        local(1, lambda a: reaction.at[a], lambda b: raw.at[3, b, mine], 7),
        local(2, lambda a: mass.at[a], lambda b: raw.at[4, b, mine], 8),
        local(3, lambda a: start.at[pl.ds(0, 3), a], lambda b: xu.at[0, :, b, mine], 9),
    ]
    first_out = pltpu.make_async_copy(start, ob.at[0], load.at[10])
    for item in stages:
        item.start()
    for item in own:
        item.start()
    first_out.start()

    barrier = pltpu.get_barrier_semaphore()

    def greet(sem, at, core):
        pl.semaphore_signal(sem, inc=1, device_id=(at, core), device_id_type=MESH)

    def near(way):
        for core in range(subs):
            greet(barrier, slab + way, core)

    greet(barrier, slab, other)
    pl.when(slab > 0)(lambda: near(-1))
    pl.when(slab < slabs - 1)(lambda: near(1))
    met = 1 + jnp.where(slab > 0, subs, 0) + jnp.where(slab < slabs - 1, subs, 0)
    steps = [1 << i for i in range((slabs - 1).bit_length())]

    def spread(i):
        d = steps[i]
        pl.when(slab + d < slabs)(lambda: greet(known.at[i, 0], slab + d, sub))
        pl.when(slab - d >= 0)(lambda: greet(known.at[i, 1], slab - d, sub))

    def gather(i):
        d = steps[i]
        pl.when(slab - d >= 0)(lambda: pl.semaphore_wait(known.at[i, 0], 1))
        pl.when(slab + d < slabs)(lambda: pl.semaphore_wait(known.at[i, 1], 1))

    def further(count):
        for _ in range(count):
            if pending:
                i = pending.pop(0)
                gather(i)
                if i + 1 < len(steps):
                    spread(i + 1)

    pending = list(range(len(steps)))

    def clear(low):
        def inner():
            zero = jnp.zeros((rows, nz), f32)
            for e in range(ITERS):
                for k in range(2):
                    xp[e, k if low else 2 + h + k] = zero
                qs[e, 1 if low else 2 + h] = zero
                y0[e, 0, 1 if low else 2 + h] = zero
                for c in range(3):
                    xu[e, c, 0 if low else 1 + h] = zero
                    y0[e, c, 0 if low else 3 + h] = zero
            for c in range(4):
                raw[c, 0 if low else 1 + h] = zero
        return inner

    pl.when(jnp.logical_not(has_left))(clear(True))
    pl.when(jnp.logical_not(has_right))(clear(False))

    row = lax.broadcasted_iota(jnp.int32, (rows, nz), 0)
    col = lax.broadcasted_iota(jnp.int32, (rows, nz), 1)
    mk[0] = jnp.where(row == rows - 1, 0.0, 1.0)
    mk[1] = jnp.where(row == 0, 0.0, 1.0)
    mk[2] = jnp.where(col == nz - 1, 0.0, 1.0)
    mk[3] = jnp.where(col == 0, 0.0, 1.0)

    def first_copy(g, kind):
        src, dst, at, w = first[g]
        if kind == 0:
            a, b = window(g, other)
            target, slot = (slab, other), 0
        elif kind == 1:
            a, b = pl.ds(cx - w, w), pl.ds(at - w, w)
            target, slot = (slab + 1, 0), 1 + sub
        else:
            a, b = pl.ds(0, w), pl.ds(at + h, w)
            target, slot = (slab - 1, subs - 1), 1 + sub
        if kind > 0 and g == 3:
            src = lambda planes: stage.at[pl.ds(1, 2), planes]
            dst = lambda planes, lines: xu.at[0, pl.ds(1, 2), planes, lines]
        return pltpu.make_async_remote_copy(
            src_ref=src(a), dst_ref=dst(b, mine), send_sem=init_send.at[g, kind],
            recv_sem=init_recv.at[g, slot], device_id=target, device_id_type=MESH,
        )

    def first_begin(g):
        if first[g][3] > 0:
            pl.when(slab < slabs - 1)(lambda: first_copy(g, 1).start())
            pl.when(slab > 0)(lambda: first_copy(g, 2).start())

    def first_wait(ref, sem):
        pltpu.make_async_copy(ref, ref, sem).wait()

    def first_near(g):
        _, dst, _, _ = first[g]
        _, b = window(g, sub)
        first_wait(dst(b, theirs), init_recv.at[g, 0])

    def first_far(g):
        _, dst, at, w = first[g]
        if g == 3:
            dst = lambda planes, lines: xu.at[0, pl.ds(1, 2), planes, lines]
        if w > 0:
            def inner():
                for r in range(subs):
                    first_wait(dst(pl.ds(0, w), pl.ds(r * cy, cy)), init_recv.at[g, 1 + r])
            pl.when(has_cross)(inner)

    def first_finish(g):
        first_copy(g, 0).wait_send()
        if first[g][3] > 0:
            pl.when(slab < slabs - 1)(lambda: first_copy(g, 1).wait_send())
            pl.when(slab > 0)(lambda: first_copy(g, 2).wait_send())

    def remote(kind, e, way):
        if kind == 0 or kind == 6:
            deep = kind // 6
            pair = (h + 1 - deep, 1 - deep) if way == 0 else (2 + deep, h + 2 + deep)
            src, dst = xp.at[e, pair[0]], xp.at[e, pair[1]]
        elif kind == 1:
            pair, pick = (h, 0) if way == 0 else (1, h + 1), pl.ds(1, 2)
            src, dst = xu.at[e, pick, pair[0]], xu.at[e, pick, pair[1]]
        elif kind == 2:
            pair = (h + 1, 1) if way == 0 else (2, h + 2)
            src, dst = qs.at[e, pair[0]], qs.at[e, pair[1]]
        elif kind == 4:
            src, dst = yq.at[e, way], y0.at[e, 0, 1 if way == 0 else h + 2]
        else:
            pair = (h, 0) if way == 0 else (3, h + 3)
            pick = 0 if kind == 3 else pl.ds(1, 2)
            src, dst = y0.at[e, pick, pair[0]], y0.at[e, pick, pair[1]]
        target = me + 1 if way == 0 else me - 1
        return pltpu.make_async_remote_copy(
            src_ref=src, dst_ref=dst, send_sem=send.at[kind, e, way], recv_sem=recv.at[kind, e, way],
            device_id=(target // subs, lax.rem(target, subs)), device_id_type=MESH,
        )

    def begin(kind, e):
        pl.when(has_right)(lambda: remote(kind, e, 0).start())
        pl.when(has_left)(lambda: remote(kind, e, 1).start())

    def arrive(kind, e):
        pl.when(has_left)(lambda: remote(kind, e, 0).wait_recv())
        pl.when(has_right)(lambda: remote(kind, e, 1).wait_recv())

    def finish(kind, e):
        pl.when(has_right)(lambda: remote(kind, e, 0).wait_send())
        pl.when(has_left)(lambda: remote(kind, e, 1).wait_send())

    lane = lax.broadcasted_iota(jnp.int32, (1, LANES), 1)

    def reduce_start(e, parts):
        line = jnp.zeros((1, LANES), f32)
        for i, part in enumerate(parts):
            line = line + jnp.where(lane == i, jnp.sum(fold(part), keepdims=True), 0.0)
        red[e, me] = line

        def tell(at, core):
            pltpu.make_async_remote_copy(
                src_ref=red.at[e, me], dst_ref=red.at[e, me],
                send_sem=red_send.at[e], recv_sem=red_recv.at[e],
                device_id=(at, core), device_id_type=MESH,
            ).start()

        def push(k, carry):
            at = lax.rem(slab + k, slabs)
            for core in range(subs):
                tell(at, core)
            return carry

        lax.fori_loop(1, slabs, push, 0)
        tell(slab, other)

    def red_wait(e, sem):
        block = red.at[e, pl.ds(0, n - 1)]
        pltpu.make_async_copy(block, block, sem.at[e]).wait()

    def reduce_end(e, count):
        red_wait(e, red_recv)
        total = jnp.sum(red[e], axis=0)
        return [
            jnp.sum(jnp.where(lane == i, total, 0.0), axis=1, keepdims=True)
            for i in range(count)
        ]

    def deliver(i, src, dst):
        planes = pl.ds(sub * h, h)
        return (
            pltpu.make_async_copy(src.at[:, :, mine], dst.at[:, planes], out_local.at[i]),
            pltpu.make_async_remote_copy(
                src_ref=src.at[:, :, theirs], dst_ref=dst.at[:, planes],
                send_sem=out_send.at[i], recv_sem=out_recv.at[i],
                device_id=(slab, other), device_id_type=MESH,
            ),
        )

    def results():
        return [deliver(e, ss.at[e], os_.at[e]) for e in range(ITERS)] + [
            deliver(ITERS + e, vv.at[e], ob.at[e + 1]) for e in range(ITERS - 1)
        ] + [deliver(2 * ITERS - 1, wl, ob.at[ITERS])]

    outs = results()

    def hand_over(i):
        for item in outs[i]:
            item.start()

    def turn(f):
        return (
            pltpu.roll(f, rows - 1, 0), pltpu.roll(f, 1, 0),
            pltpu.roll(f, nz - 1, 1), pltpu.roll(f, 1, 1),
        )

    def masked(f):
        yp, ym, zp, zm = turn(f)
        return yp * mk[0], ym * mk[1], zp * mk[2], zm * mk[3]

    def off_diagonal(below, around, above, k):
        yp, ym, zp, zm = around
        total = co[0, k] * above + co[1, k] * below
        total = total + (co[2, k] * yp + co[3, k] * ym)
        return total + (co[4, k] * zp + co[5, k] * zm)

    def inside(k):
        at = me * h + k
        return jnp.where(jnp.logical_and(at >= 0, at < n * h), 1.0, 0.0)

    def coefficients(k, carry):
        hx, hy, hz = 0.5 * raw[0, k], 0.5 * raw[1, k], 0.5 * raw[2, k]
        co[0, k] = 1.0 - hx
        co[1, k] = 1.0 + hx
        co[2, k] = (1.0 - hy) * mk[0]
        co[3, k] = (1.0 + hy) * mk[1]
        co[4, k] = (1.0 - hz) * mk[2]
        co[5, k] = (1.0 + hz) * mk[3]
        diagonal = 6.0 + raw[3, k]
        co[6, k] = diagonal
        co[7, k] = inside(k - 1) / diagonal
        return carry

    def masses(k, carry):
        co[8, k] = 1.0 / raw[4, k]
        return carry

    def guess_own(e):
        for k in range(1, h + 1):
            here = xp[e, k + 1]
            yp, ym, zp, zm = masked(here)
            total = (yp + ym) + (zp + zm)
            if k > 1:
                total = total + xp[e, k]
            if k < h:
                total = total + xp[e, k + 2]
            t1[k] = (here + total * (1.0 / 7.0)) * (1.0 / 7.0)

    def guess_rest(e):
        t1[1] = t1[1] + xp[e, 1] * (1.0 / 49.0)
        t1[h] = t1[h] + xp[e, h + 2] * (1.0 / 49.0)
        for k in (0, h + 1):
            guess(e)(k, 0)

    def guess(e):
        def body(k, carry):
            here = xp[e, k + 1]
            yp, ym, zp, zm = masked(here)
            total = (xp[e, k] + xp[e, k + 2]) + (yp + ym) + (zp + zm)
            t1[k] = (here + total * (1.0 / 7.0)) * (inside(k - 1) * (1.0 / 7.0))
            return carry
        return body

    def schur(e):
        def body(k, carry):
            here = t1[k + 1]
            off = off_diagonal(t1[k], turn(here), t1[k + 2], k + 1)
            qs[e, k + 2] = (off - co[6, k + 1] * here) * co[8, k + 1]
            return carry
        return body

    def velocity_along(e, k):
        found = xu[e, 0, k + 1] - 0.5 * (qs[e, k + 3] - qs[e, k + 1])
        y0[e, 0, k + 2] = found * co[7, k + 1]

    def velocity_across(e):
        def body(k, carry):
            yp, ym, zp, zm = masked(qs[e, k + 2])
            scale = co[7, k + 1]
            y0[e, 1, k + 2] = (xu[e, 1, k + 1] - 0.5 * (yp - ym)) * scale
            y0[e, 2, k + 2] = (xu[e, 2, k + 1] - 0.5 * (zp - zm)) * scale
            return carry
        return body

    def second(e, c, k, skip=None):
        yp, ym, zp, zm = turn(y0[e, c, k + 2])
        off = (co[2, k + 1] * yp + co[3, k + 1] * ym) + (co[4, k + 1] * zp + co[5, k + 1] * zm)
        if skip != 0:
            off = off + co[0, k + 1] * y0[e, c, k + 3]
        if skip != 1:
            off = off + co[1, k + 1] * y0[e, c, k + 1]
        z1[c, k + 1] = off * co[7, k + 1]

    def second_across(e):
        for c in (1, 2):
            for k in range(h):
                second(e, c, k, 1 if k == 0 else 0 if k == h - 1 else None)

    def across(e, k):
        one, two = y0[e, 1, k + 2] + z1[1, k + 1], y0[e, 2, k + 2] + z1[2, k + 1]
        a, b = pltpu.roll(one, rows - 1, 0), pltpu.roll(one, 1, 0)
        found = a * mk[0] - b * mk[1]
        a, b = pltpu.roll(two, nz - 1, 1), pltpu.roll(two, 1, 1)
        return 0.5 * (found + (a * mk[2] - b * mk[3]))

    def low_own(e):
        for k in range(h):
            q = qs[e, k + 2]
            yp, ym, zp, zm = masked(q)
            total = (yp + ym) + (zp + zm)
            if k > 0:
                total = total + qs[e, k + 1]
            if k < h - 1:
                total = total + qs[e, k + 3]
            total = 0.5 * total - 3.0 * q
            if 0 < k < h - 1:
                total = total - across(e, k)
            t1[k + 1] = total

    def velocity_share(e):
        yq[e, 0] = (xu[e, 0, h] + 0.5 * qs[e, h]) * co[7, h]
        yq[e, 1] = (xu[e, 0, 1] - 0.5 * qs[e, 3]) * co[7, 1]

    def velocity_edges(e):
        for k, near, sign in ((-1, 2, -0.5), (h, h + 1, 0.5)):
            yp, ym, zp, zm = masked(qs[e, k + 2])
            scale = co[7, k + 1]
            y0[e, 0, k + 2] = y0[e, 0, k + 2] + (sign * qs[e, near]) * scale
            y0[e, 1, k + 2] = (xu[e, 1, k + 1] - 0.5 * (yp - ym)) * scale
            y0[e, 2, k + 2] = (xu[e, 2, k + 1] - 0.5 * (zp - zm)) * scale

    def second_rest(e):
        for c in (1, 2):
            z1[c, 1] = z1[c, 1] + co[1, 1] * y0[e, c, 1] * co[7, 1]
            z1[c, h] = z1[c, h] + co[0, h] * y0[e, c, h + 2] * co[7, h]
        for k in range(h):
            second(e, 0, k)
        second_edges(e, 0)

    def second_edges(e, c):
        second(e, c, -1, 1)
        second(e, c, h, 0)

    def mixer(e, factor, weights):
        def mix(value, held):
            if e > 0:
                value = value * factor
                for g, item in zip(weights, held):
                    value = value - g * item
            return value
        return mix

    def image_low(e, factor, weights):
        mix = mixer(e, factor, weights)
        full = [y0[e, 0, k + 2] + z1[0, k + 1] for k in range(-1, h + 1)]
        for k in range(h):
            low = t1[k + 1] - 0.5 * (full[k + 2] - full[k])
            if k == 0:
                low = low + 0.5 * qs[e, 1]
            if k == h - 1:
                low = low + 0.5 * qs[e, h + 2]
            if k == 0 or k == h - 1:
                low = low - across(e, k)
            value = mix(low, [xp[i + 1, k + 2] for i in range(e)])
            if e + 1 < ITERS:
                xp[e + 1, k + 2] = value
            else:
                wl[3, k] = value

    def image(e, factor, weights):
        mix = mixer(e, factor, weights)

        def body(k, carry):
            for c in range(3):
                here = z1[c, k + 1]
                off = off_diagonal(z1[c, k], turn(here), z1[c, k + 2], k + 1)
                value = mix(xu[e, c, k + 1] - off, [xu[i + 1, c, k + 1] for i in range(e)])
                ss[e, c, k] = mix(y0[e, c, k + 2] + here, [ss[i, c, k] for i in range(e)])
                if e + 1 < ITERS:
                    xu[e + 1, c, k + 1] = value
                else:
                    wl[c, k] = value
            ss[e, 3, k] = mix(qs[e, k + 2], [ss[i, 3, k] for i in range(e)])
            return carry
        return body

    def held_of(i, c, k):
        if i > 0:
            return vv[i - 1, c, k]
        return xp[0, k + 2] if c == 3 else xu[0, c, k + 1]

    def image_of(e, c, k):
        if e + 1 == ITERS:
            return wl[c, k]
        return xp[e + 1, k + 2] if c == 3 else xu[e + 1, c, k + 1]

    stages[0].wait()
    pl.semaphore_wait(barrier, met)
    first_begin(0)
    first_copy(0, 0).start()
    spread(0)
    for item in stages[1:4]:
        item.wait()
    first_begin(1)
    first_copy(1, 0).start()
    first_copy(2, 0).start()
    stages[4].wait()
    first_begin(3)
    first_copy(3, 0).start()
    for item in own[1:4]:
        item.wait()
    first_near(1)
    first_near(2)
    loop(h, coefficients, low=1)
    loop(h, masses, low=1)
    further(1)
    own[0].wait()
    first_near(0)
    guess_own(0)
    first_far(0)

    zero = jnp.zeros((rows, nz), f32)
    inverses, entries = [], {}
    factor, weights = None, []
    for e in range(ITERS):
        if e > 0:
            arrive(6, e)
            arrive(0, e)
        guess_rest(e)
        loop(h, schur(e))
        begin(2, e)
        if e == 0:
            further(1)
            own[4].wait()
            first_near(3)
        velocity_share(e)
        begin(4, e)
        for k in range(1, h - 1):
            velocity_along(e, k)
        begin(3, e)
        loop(h, velocity_across(e))
        begin(5, e)
        second_across(e)
        low_own(e)
        if e == 0:
            first_far(1)
            coefficients(0, 0)
            coefficients(h + 1, 0)
            ca[0] = co[1, 0] * co[7, 0]
            ca[1] = co[0, h + 1] * co[7, h + 1]
            ca[2] = co[1, 1] * ca[0]
            ca[3] = co[0, h] * ca[1]
            first_far(3)
            further(1)
        else:
            sums = reduce_end(e - 1, e + 1)
            norm = jnp.sqrt(sums[0])
            factor = 1.0 / norm
            if e > 1:
                entries[(e - 1, e - 2)] = norm
            inverses.append(factor)
            weights = []
            for i in range(e):
                value = sums[i + 1] * inverses[i] * factor
                entries[(i, e - 1)] = value
                weights.append(value * inverses[i])

            def form(k, carry, e=e):
                for c in range(4):
                    value = image_of(e - 1, c, k) * factor
                    for i in range(e):
                        value = value - weights[i] * held_of(i, c, k)
                    vv[e - 1, c, k] = value
                return carry

            loop(h, form)
            hand_over(ITERS + e - 1)
            arrive(1, e)
        arrive(2, e)
        velocity_along(e, 0)
        velocity_along(e, h - 1)
        arrive(4, e)
        velocity_edges(e)
        second_rest(e)
        image_low(e, factor, weights)
        if e + 1 < ITERS:
            begin(6, e + 1)
        arrive(3, e)

        scale = factor if e > 0 else 1.0

        def beyond(c, e=e, scale=scale):
            return y0[e, c, 0] * scale, y0[e, c, h + 3] * scale

        below, above = beyond(0)
        if e + 1 < ITERS:
            xp[e + 1, 2] = xp[e + 1, 2] + 0.5 * (ca[0] * below)
            xp[e + 1, h + 1] = xp[e + 1, h + 1] - 0.5 * (ca[1] * above)
            begin(0, e + 1)
        else:
            wl[3, 0] = wl[3, 0] + 0.5 * (ca[0] * below)
            wl[3, h - 1] = wl[3, h - 1] - 0.5 * (ca[1] * above)
        second_edges(e, 1)
        second_edges(e, 2)
        loop(h, image(e, factor, weights))
        hand_over(e)
        if e == 0:
            further(len(steps))
        arrive(5, e)
        for c in range(3):
            below, above = beyond(c)
            if e + 1 < ITERS:
                xu[e + 1, c, 1] = xu[e + 1, c, 1] - ca[2] * below
                xu[e + 1, c, h] = xu[e + 1, c, h] - ca[3] * above
            else:
                wl[c, 0] = wl[c, 0] - ca[2] * below
                wl[c, h - 1] = wl[c, h - 1] - ca[3] * above
        if e + 1 == ITERS:
            hand_over(2 * ITERS - 1)

        def totals(k, acc, e=e):
            acc = list(acc)
            found = [image_of(e, c, k) for c in range(4)]
            for i in range(e + 1):
                held = [held_of(i, c, k) for c in range(4)]
                term = held[0] * found[0] + held[1] * found[1]
                acc[i + 1] = acc[i + 1] + (term + (held[2] * found[2] + held[3] * found[3]))
                if i == e:
                    term = held[0] * held[0] + held[1] * held[1]
                    acc[0] = acc[0] + (term + (held[2] * held[2] + held[3] * held[3]))
            if e + 1 == ITERS:
                term = found[0] * found[0] + found[1] * found[1]
                acc[e + 2] = acc[e + 2] + (term + (found[2] * found[2] + found[3] * found[3]))
            return tuple(acc)

        count = e + 2 if e + 1 < ITERS else e + 3
        reduce_start(e, loop(h, totals, (zero,) * count))
        if e + 1 < ITERS:
            begin(1, e + 1)
            guess_own(e + 1)

    for g in range(len(first)):
        first_finish(g)
    first_out.wait()
    for e in range(ITERS):
        for kind in range(7):
            if e > 0 or kind in (2, 3, 4, 5):
                finish(kind, e)
    for here, there in outs:
        here.wait()
        there.wait()
    for e in range(ITERS - 1):
        red_wait(e, red_send)
    sums = reduce_end(ITERS - 1, ITERS + 2)
    norm = jnp.sqrt(sums[0])
    factor = 1.0 / norm
    entries[(ITERS - 1, ITERS - 2)] = norm
    inverses.append(factor)
    left = sums[ITERS + 1] * factor * factor
    spread = []
    for i in range(ITERS):
        value = sums[i + 1] * inverses[i] * factor
        entries[(i, ITERS - 1)] = value
        spread.append(value * inverses[i])
        left = left - value * value
    norm = jnp.sqrt(left)
    entries[(ITERS, ITERS - 1)] = norm
    inverse = 1.0 / norm
    lines = inverses + [factor * inverse] + [g * inverse for g in spread]
    for i, value in enumerate(lines):
        scal[i : i + 1] = jnp.broadcast_to(value, (1, LANES))
    r = lax.broadcasted_iota(jnp.int32, (8, LANES), 0)
    c = lax.broadcasted_iota(jnp.int32, (8, LANES), 1)
    table = jnp.zeros((8, LANES), f32)
    for (i, j), value in entries.items():
        table = table + jnp.where(jnp.logical_and(r == i, c == j), value, 0.0)
    scal[8:16] = table
    red_wait(ITERS - 1, red_send)


def write(ob, os_, scal, basis, search, hess, bb, sb, hb, sems):
    def value(i):
        return scal[i : i + 1, 0:1]

    copies = []

    def emit(src, dst, i):
        item = pltpu.make_async_copy(src, dst, sems.at[i])
        item.start()
        copies.append(item)

    hb[...] = scal[8 : 8 + ITERS + 1, 0:ITERS]
    emit(hb, hess, 2 * ITERS + 1)
    planes = ob.shape[2]
    inverse = [value(i) for i in range(ITERS)]
    for e in range(ITERS):
        def body(k, carry, e=e):
            for c in range(4):
                bb[e, c, k] = ob[e, c, k] * inverse[e]
                sb[e, c, k] = os_[e, c, k] * inverse[e]
            return carry

        loop(planes, body)
        emit(bb.at[e], basis.at[e], e)
        emit(sb.at[e], search.at[e], ITERS + 1 + e)
    weights = [value(ITERS + i) for i in range(ITERS + 1)]

    def last(k, carry):
        for c in range(4):
            total = ob[ITERS, c, k] * weights[0]
            for i in range(ITERS):
                total = total - weights[i + 1] * ob[i, c, k]
            bb[ITERS, c, k] = total
        return carry

    loop(planes, last)
    emit(bb.at[ITERS], basis.at[ITERS], ITERS)
    for item in copies:
        item.wait()


def per_device(slabs, subs, start, wind, reaction, mass):
    _, cx, cy, nz = start.shape
    n = slabs * subs
    rows, h = subs * cy, cx // subs
    assert subs == 2 and cx % subs == 0 and h >= 3
    f32 = jnp.float32

    def field(*lead):
        return pltpu.VMEM((*lead, rows, nz), f32)

    anywhere = pl.BlockSpec(memory_space=pl.ANY)
    vmem = pl.BlockSpec(memory_space=pltpu.VMEM)
    hbm = pl.BlockSpec(memory_space=pltpu.HBM)
    ob, os_, scal = pl.pallas_call(
        functools.partial(kernel, slabs, subs, cx, cy, nz),
        out_shape=(
            jax.ShapeDtypeStruct((ITERS + 1, 4, cx, cy, nz), f32),
            jax.ShapeDtypeStruct((ITERS, 4, cx, cy, nz), f32),
            jax.ShapeDtypeStruct((16, LANES), f32),
        ),
        in_specs=[hbm] * 4,
        out_specs=(anywhere, anywhere, vmem),
        scratch_shapes=[
            pltpu.VMEM((9, cx, cy, nz), f32),
            field(ITERS, h + 4),
            field(ITERS, 3, h + 2),
            field(ITERS, h + 4),
            field(ITERS, 3, h + 4),
            field(ITERS, 2),
            field(h + 2),
            field(3, h + 2),
            field(5, h + 2),
            field(9, h + 2),
            field(4),
            field(4),
            field(ITERS - 1, 4, h),
            field(ITERS, 4, h),
            field(4, h),
            pltpu.VMEM((ITERS, n, 1, LANES), f32),
            pltpu.SemaphoreType.DMA((4, 3)),
            pltpu.SemaphoreType.DMA((4, 3)),
            pltpu.SemaphoreType.DMA((7, ITERS, 2)),
            pltpu.SemaphoreType.DMA((7, ITERS, 2)),
            pltpu.SemaphoreType.DMA((ITERS,)),
            pltpu.SemaphoreType.DMA((ITERS,)),
            pltpu.SemaphoreType.DMA((11,)),
            pltpu.SemaphoreType.DMA((2 * ITERS,)),
            pltpu.SemaphoreType.DMA((2 * ITERS,)),
            pltpu.SemaphoreType.DMA((2 * ITERS,)),
            pltpu.SemaphoreType.REGULAR(((slabs - 1).bit_length(), 2)),
        ],
        compiler_params=pltpu.CompilerParams(
            collective_id=0, has_side_effects=True, vmem_limit_bytes=40_000_000
        ),
    )(*(pltpu.with_memory_space_constraint(x, pltpu.HBM) for x in (start, wind, reaction, mass)))
    return pl.pallas_call(
        write,
        out_shape=(
            jax.ShapeDtypeStruct((ITERS + 1, 4, cx, cy, nz), f32),
            jax.ShapeDtypeStruct((ITERS, 4, cx, cy, nz), f32),
            jax.ShapeDtypeStruct((ITERS + 1, ITERS), f32),
        ),
        in_specs=[vmem] * 3,
        out_specs=(hbm, hbm, hbm),
        scratch_shapes=[
            pltpu.VMEM((ITERS + 1, 4, cx, cy, nz), f32),
            pltpu.VMEM((ITERS, 4, cx, cy, nz), f32),
            pltpu.VMEM((ITERS + 1, ITERS), f32),
            pltpu.SemaphoreType.DMA((2 * ITERS + 2,)),
        ],
        compiler_params=pltpu.CompilerParams(vmem_limit_bytes=10_000_000),
    )(ob, os_, scal)


def solution(mesh):
    slabs, subs = mesh.shape["slab"], mesh.shape["sub"]
    return jax.shard_map(
        functools.partial(per_device, slabs, subs),
        mesh=mesh,
        in_specs=(
            P(None, "slab", "sub", None),
            P(None, "slab", "sub", None),
            P("slab", "sub", None),
            P("slab", "sub", None),
        ),
        out_specs=(P(None, None, "slab", "sub", None), P(None, None, "slab", "sub", None), P()),
        check_vma=False,
    )
```

```python
import functools

import jax
import jax.numpy as jnp
from jax import lax
from jax.experimental import pallas as pl
from jax.experimental.pallas import tpu as pltpu
from jax.sharding import PartitionSpec as P

ITERS = 3
UNROLL = 6
LANES = 128
MESH = pl.DeviceIdType.MESH


def fold(x):
    rows, cols = x.shape
    total = None
    for r in range(0, rows, 8):
        for c in range(0, cols, LANES):
            piece = x[r : r + 8, c : c + LANES]
            total = piece if total is None else total + piece
    return total


def loop(count, body, init=0, low=0):
    step = max(u for u in range(1, UNROLL + 1) if count % u == 0)

    def several(k, carry):
        for i in range(step):
            carry = body(low + k * step + i, carry)
        return carry

    return lax.fori_loop(0, count // step, several, init)


def kernel(
    slabs, subs, cx, cy, nz,
    start, wind, reaction, mass, ob, os_, scal,
    stage, xp, xu, qs, y0, yq, t1, z1, raw, co, ca, mk, vv, ss, wl, red,
    init_send, init_recv, send, recv, red_send, red_recv, load, out_local, out_send, out_recv, known,
):
    slab, sub = lax.axis_index("slab"), lax.axis_index("sub")
    n = slabs * subs
    me = slab * subs + sub
    h = cx // subs
    rows = subs * cy
    f32 = jnp.float32
    other = 1 - sub
    has_left, has_right = me > 0, me < n - 1
    has_cross = jnp.where(sub == 0, slab, slabs - 1 - slab) > 0
    mine = pl.ds(pl.multiple_of(sub * cy, 8), cy)
    theirs = pl.ds(pl.multiple_of(other * cy, 8), cy)

    def staged(lo, count):
        return lambda planes: stage.at[pl.ds(lo, count), planes]

    first = [
        (lambda planes: stage.at[3, planes], lambda planes, lines: xp.at[0, planes, lines], 2, 2),
        (staged(4, 4), lambda planes, lines: raw.at[pl.ds(0, 4), planes, lines], 1, 1),
        (lambda planes: stage.at[8, planes], lambda planes, lines: raw.at[4, planes, lines], 1, 0),
        (staged(0, 3), lambda planes, lines: xu.at[0, :, planes, lines], 1, 1),
    ]

    def window(g, side):
        _, _, at, w = first[g]
        return pl.ds(side * (h - w), h + w), pl.ds(at - side * w, h + w)

    def local(g, src, dst, sem):
        a, b = window(g, sub)
        return pltpu.make_async_copy(src(a), dst(b), load.at[sem])

    stages = [
        pltpu.make_async_copy(start.at[3], stage.at[3], load.at[0]),
        pltpu.make_async_copy(wind, stage.at[pl.ds(4, 3)], load.at[1]),
        pltpu.make_async_copy(reaction, stage.at[7], load.at[2]),
        pltpu.make_async_copy(mass, stage.at[8], load.at[3]),
        pltpu.make_async_copy(start.at[pl.ds(0, 3)], stage.at[pl.ds(0, 3)], load.at[4]),
    ]
    own = [
        local(0, lambda a: start.at[3, a], lambda b: xp.at[0, b, mine], 5),
        local(1, lambda a: wind.at[:, a], lambda b: raw.at[pl.ds(0, 3), b, mine], 6),
        local(1, lambda a: reaction.at[a], lambda b: raw.at[3, b, mine], 7),
        local(2, lambda a: mass.at[a], lambda b: raw.at[4, b, mine], 8),
        local(3, lambda a: start.at[pl.ds(0, 3), a], lambda b: xu.at[0, :, b, mine], 9),
    ]
    first_out = pltpu.make_async_copy(start, ob.at[0], load.at[10])
    for item in stages:
        item.start()
    for item in own:
        item.start()
    first_out.start()

    barrier = pltpu.get_barrier_semaphore()

    def greet(sem, at, core):
        pl.semaphore_signal(sem, inc=1, device_id=(at, core), device_id_type=MESH)

    def near(way):
        for core in range(subs):
            greet(barrier, slab + way, core)

    greet(barrier, slab, other)
    pl.when(slab > 0)(lambda: near(-1))
    pl.when(slab < slabs - 1)(lambda: near(1))
    met = 1 + jnp.where(slab > 0, subs, 0) + jnp.where(slab < slabs - 1, subs, 0)
    steps = [1 << i for i in range((slabs - 1).bit_length())]

    def spread(i):
        d = steps[i]
        pl.when(slab + d < slabs)(lambda: greet(known.at[i, 0], slab + d, sub))
        pl.when(slab - d >= 0)(lambda: greet(known.at[i, 1], slab - d, sub))

    def gather(i):
        d = steps[i]
        pl.when(slab - d >= 0)(lambda: pl.semaphore_wait(known.at[i, 0], 1))
        pl.when(slab + d < slabs)(lambda: pl.semaphore_wait(known.at[i, 1], 1))

    def further(count):
        for _ in range(count):
            if pending:
                i = pending.pop(0)
                gather(i)
                if i + 1 < len(steps):
                    spread(i + 1)

    pending = list(range(len(steps)))

    def clear(low):
        def inner():
            zero = jnp.zeros((rows, nz), f32)
            for e in range(ITERS):
                for k in range(2):
                    xp[e, k if low else 2 + h + k] = zero
                qs[e, 1 if low else 2 + h] = zero
                y0[e, 0, 1 if low else 2 + h] = zero
                for c in range(3):
                    xu[e, c, 0 if low else 1 + h] = zero
                    y0[e, c, 0 if low else 3 + h] = zero
            for c in range(4):
                raw[c, 0 if low else 1 + h] = zero
        return inner

    pl.when(jnp.logical_not(has_left))(clear(True))
    pl.when(jnp.logical_not(has_right))(clear(False))

    row = lax.broadcasted_iota(jnp.int32, (rows, nz), 0)
    col = lax.broadcasted_iota(jnp.int32, (rows, nz), 1)
    mk[0] = jnp.where(row == rows - 1, 0.0, 1.0)
    mk[1] = jnp.where(row == 0, 0.0, 1.0)
    mk[2] = jnp.where(col == nz - 1, 0.0, 1.0)
    mk[3] = jnp.where(col == 0, 0.0, 1.0)

    def first_copy(g, kind):
        src, dst, at, w = first[g]
        if kind == 0:
            a, b = window(g, other)
            target, slot = (slab, other), 0
        elif kind == 1:
            a, b = pl.ds(cx - w, w), pl.ds(at - w, w)
            target, slot = (slab + 1, 0), 1 + sub
        else:
            a, b = pl.ds(0, w), pl.ds(at + h, w)
            target, slot = (slab - 1, subs - 1), 1 + sub
        if kind > 0 and g == 3:
            src = lambda planes: stage.at[pl.ds(1, 2), planes]
            dst = lambda planes, lines: xu.at[0, pl.ds(1, 2), planes, lines]
        return pltpu.make_async_remote_copy(
            src_ref=src(a), dst_ref=dst(b, mine), send_sem=init_send.at[g, kind],
            recv_sem=init_recv.at[g, slot], device_id=target, device_id_type=MESH,
        )

    def first_begin(g):
        if first[g][3] > 0:
            pl.when(slab < slabs - 1)(lambda: first_copy(g, 1).start())
            pl.when(slab > 0)(lambda: first_copy(g, 2).start())

    def first_wait(ref, sem):
        pltpu.make_async_copy(ref, ref, sem).wait()

    def first_near(g):
        _, dst, _, _ = first[g]
        _, b = window(g, sub)
        first_wait(dst(b, theirs), init_recv.at[g, 0])

    def first_far(g):
        _, dst, at, w = first[g]
        if g == 3:
            dst = lambda planes, lines: xu.at[0, pl.ds(1, 2), planes, lines]
        if w > 0:
            def inner():
                for r in range(subs):
                    first_wait(dst(pl.ds(0, w), pl.ds(r * cy, cy)), init_recv.at[g, 1 + r])
            pl.when(has_cross)(inner)

    def first_finish(g):
        first_copy(g, 0).wait_send()
        if first[g][3] > 0:
            pl.when(slab < slabs - 1)(lambda: first_copy(g, 1).wait_send())
            pl.when(slab > 0)(lambda: first_copy(g, 2).wait_send())

    def remote(kind, e, way):
        if kind == 0 or kind == 6:
            deep = kind // 6
            pair = (h + 1 - deep, 1 - deep) if way == 0 else (2 + deep, h + 2 + deep)
            src, dst = xp.at[e, pair[0]], xp.at[e, pair[1]]
        elif kind == 1:
            pair, pick = (h, 0) if way == 0 else (1, h + 1), pl.ds(1, 2)
            src, dst = xu.at[e, pick, pair[0]], xu.at[e, pick, pair[1]]
        elif kind == 2:
            pair = (h + 1, 1) if way == 0 else (2, h + 2)
            src, dst = qs.at[e, pair[0]], qs.at[e, pair[1]]
        elif kind == 4:
            src, dst = yq.at[e, way], y0.at[e, 0, 1 if way == 0 else h + 2]
        else:
            pair = (h, 0) if way == 0 else (3, h + 3)
            pick = 0 if kind == 3 else pl.ds(1, 2)
            src, dst = y0.at[e, pick, pair[0]], y0.at[e, pick, pair[1]]
        target = me + 1 if way == 0 else me - 1
        return pltpu.make_async_remote_copy(
            src_ref=src, dst_ref=dst, send_sem=send.at[kind, e, way], recv_sem=recv.at[kind, e, way],
            device_id=(target // subs, lax.rem(target, subs)), device_id_type=MESH,
        )

    def begin(kind, e):
        pl.when(has_right)(lambda: remote(kind, e, 0).start())
        pl.when(has_left)(lambda: remote(kind, e, 1).start())

    def arrive(kind, e):
        pl.when(has_left)(lambda: remote(kind, e, 0).wait_recv())
        pl.when(has_right)(lambda: remote(kind, e, 1).wait_recv())

    def finish(kind, e):
        pl.when(has_right)(lambda: remote(kind, e, 0).wait_send())
        pl.when(has_left)(lambda: remote(kind, e, 1).wait_send())

    lane = lax.broadcasted_iota(jnp.int32, (1, LANES), 1)

    def reduce_start(e, parts):
        line = jnp.zeros((1, LANES), f32)
        for i, part in enumerate(parts):
            line = line + jnp.where(lane == i, jnp.sum(fold(part), keepdims=True), 0.0)
        red[e, me] = line

        def tell(at, core):
            pltpu.make_async_remote_copy(
                src_ref=red.at[e, me], dst_ref=red.at[e, me],
                send_sem=red_send.at[e], recv_sem=red_recv.at[e],
                device_id=(at, core), device_id_type=MESH,
            ).start()

        def push(k, carry):
            at = lax.rem(slab + k, slabs)
            for core in range(subs):
                tell(at, core)
            return carry

        lax.fori_loop(1, slabs, push, 0)
        tell(slab, other)

    def red_wait(e, sem):
        block = red.at[e, pl.ds(0, n - 1)]
        pltpu.make_async_copy(block, block, sem.at[e]).wait()

    def reduce_end(e, count):
        red_wait(e, red_recv)
        total = jnp.sum(red[e], axis=0)
        return [
            jnp.sum(jnp.where(lane == i, total, 0.0), axis=1, keepdims=True)
            for i in range(count)
        ]

    def deliver(i, src, dst):
        planes = pl.ds(sub * h, h)
        return (
            pltpu.make_async_copy(src.at[:, :, mine], dst.at[:, planes], out_local.at[i]),
            pltpu.make_async_remote_copy(
                src_ref=src.at[:, :, theirs], dst_ref=dst.at[:, planes],
                send_sem=out_send.at[i], recv_sem=out_recv.at[i],
                device_id=(slab, other), device_id_type=MESH,
            ),
        )

    def results():
        return [deliver(e, ss.at[e], os_.at[e]) for e in range(ITERS)] + [
            deliver(ITERS + e, vv.at[e], ob.at[e + 1]) for e in range(ITERS - 1)
        ] + [deliver(2 * ITERS - 1, wl, ob.at[ITERS])]

    outs = results()

    def hand_over(i):
        for item in outs[i]:
            item.start()

    def turn(f):
        return (
            pltpu.roll(f, rows - 1, 0), pltpu.roll(f, 1, 0),
            pltpu.roll(f, nz - 1, 1), pltpu.roll(f, 1, 1),
        )

    def masked(f):
        yp, ym, zp, zm = turn(f)
        return yp * mk[0], ym * mk[1], zp * mk[2], zm * mk[3]

    def off_diagonal(below, around, above, k):
        yp, ym, zp, zm = around
        total = co[0, k] * above + co[1, k] * below
        total = total + (co[2, k] * yp + co[3, k] * ym)
        return total + (co[4, k] * zp + co[5, k] * zm)

    def inside(k):
        at = me * h + k
        return jnp.where(jnp.logical_and(at >= 0, at < n * h), 1.0, 0.0)

    def coefficients(k, carry):
        hx, hy, hz = 0.5 * raw[0, k], 0.5 * raw[1, k], 0.5 * raw[2, k]
        co[0, k] = 1.0 - hx
        co[1, k] = 1.0 + hx
        co[2, k] = (1.0 - hy) * mk[0]
        co[3, k] = (1.0 + hy) * mk[1]
        co[4, k] = (1.0 - hz) * mk[2]
        co[5, k] = (1.0 + hz) * mk[3]
        diagonal = 6.0 + raw[3, k]
        co[6, k] = diagonal
        co[7, k] = inside(k - 1) / diagonal
        return carry

    def masses(k, carry):
        co[8, k] = 1.0 / raw[4, k]
        return carry

    def guess_own(e):
        for k in range(1, h + 1):
            here = xp[e, k + 1]
            yp, ym, zp, zm = masked(here)
            total = (yp + ym) + (zp + zm)
            if k > 1:
                total = total + xp[e, k]
            if k < h:
                total = total + xp[e, k + 2]
            t1[k] = (here + total * (1.0 / 7.0)) * (1.0 / 7.0)

    def guess_rest(e):
        t1[1] = t1[1] + xp[e, 1] * (1.0 / 49.0)
        t1[h] = t1[h] + xp[e, h + 2] * (1.0 / 49.0)
        for k in (0, h + 1):
            guess(e)(k, 0)

    def guess(e):
        def body(k, carry):
            here = xp[e, k + 1]
            yp, ym, zp, zm = masked(here)
            total = (xp[e, k] + xp[e, k + 2]) + (yp + ym) + (zp + zm)
            t1[k] = (here + total * (1.0 / 7.0)) * (inside(k - 1) * (1.0 / 7.0))
            return carry
        return body

    def schur(e):
        def body(k, carry):
            here = t1[k + 1]
            off = off_diagonal(t1[k], turn(here), t1[k + 2], k + 1)
            qs[e, k + 2] = (off - co[6, k + 1] * here) * co[8, k + 1]
            return carry
        return body

    def velocity_along(e, k):
        found = xu[e, 0, k + 1] - 0.5 * (qs[e, k + 3] - qs[e, k + 1])
        y0[e, 0, k + 2] = found * co[7, k + 1]

    def velocity_across(e):
        def body(k, carry):
            yp, ym, zp, zm = masked(qs[e, k + 2])
            scale = co[7, k + 1]
            y0[e, 1, k + 2] = (xu[e, 1, k + 1] - 0.5 * (yp - ym)) * scale
            y0[e, 2, k + 2] = (xu[e, 2, k + 1] - 0.5 * (zp - zm)) * scale
            return carry
        return body

    def second(e, c, k, skip=None):
        yp, ym, zp, zm = turn(y0[e, c, k + 2])
        off = (co[2, k + 1] * yp + co[3, k + 1] * ym) + (co[4, k + 1] * zp + co[5, k + 1] * zm)
        if skip != 0:
            off = off + co[0, k + 1] * y0[e, c, k + 3]
        if skip != 1:
            off = off + co[1, k + 1] * y0[e, c, k + 1]
        z1[c, k + 1] = off * co[7, k + 1]

    def second_across(e):
        for c in (1, 2):
            for k in range(h):
                second(e, c, k, 1 if k == 0 else 0 if k == h - 1 else None)

    def across(e, k):
        one, two = y0[e, 1, k + 2] + z1[1, k + 1], y0[e, 2, k + 2] + z1[2, k + 1]
        a, b = pltpu.roll(one, rows - 1, 0), pltpu.roll(one, 1, 0)
        found = a * mk[0] - b * mk[1]
        a, b = pltpu.roll(two, nz - 1, 1), pltpu.roll(two, 1, 1)
        return 0.5 * (found + (a * mk[2] - b * mk[3]))

    def low_own(e):
        for k in range(h):
            q = qs[e, k + 2]
            yp, ym, zp, zm = masked(q)
            total = (yp + ym) + (zp + zm)
            if k > 0:
                total = total + qs[e, k + 1]
            if k < h - 1:
                total = total + qs[e, k + 3]
            total = 0.5 * total - 3.0 * q
            if 0 < k < h - 1:
                total = total - across(e, k)
            t1[k + 1] = total

    def velocity_share(e):
        yq[e, 0] = (xu[e, 0, h] + 0.5 * qs[e, h]) * co[7, h]
        yq[e, 1] = (xu[e, 0, 1] - 0.5 * qs[e, 3]) * co[7, 1]

    def near_across(e):
        for k in (-1, h):
            velocity_across(e)(k, 0)
        for c in (1, 2):
            z1[c, 1] = z1[c, 1] + co[1, 1] * y0[e, c, 1] * co[7, 1]
            z1[c, h] = z1[c, h] + co[0, h] * y0[e, c, h + 2] * co[7, h]
        for k in range(h):
            second(e, 0, k, 1 if k == 0 else 0 if k == h - 1 else None)
        t1[1] = t1[1] + 0.5 * qs[e, 1] - across(e, 0)
        t1[h] = t1[h] + 0.5 * qs[e, h + 2] - across(e, h - 1)

    def near_along(e):
        for k, near, sign in ((-1, 2, -0.5), (h, h + 1, 0.5)):
            y0[e, 0, k + 2] = y0[e, 0, k + 2] + (sign * qs[e, near]) * co[7, k + 1]
        z1[0, 1] = z1[0, 1] + co[1, 1] * y0[e, 0, 1] * co[7, 1]
        z1[0, h] = z1[0, h] + co[0, h] * y0[e, 0, h + 2] * co[7, h]
        second_edges(e, 0)

    def second_edges(e, c):
        second(e, c, -1, 1)
        second(e, c, h, 0)

    def mixer(e, factor, weights):
        def mix(value, held):
            if e > 0:
                value = value * factor
                for g, item in zip(weights, held):
                    value = value - g * item
            return value
        return mix

    def image_low(e, factor, weights):
        mix = mixer(e, factor, weights)
        full = [y0[e, 0, k + 2] + z1[0, k + 1] for k in range(-1, h + 1)]
        for k in range(h):
            low = t1[k + 1] - 0.5 * (full[k + 2] - full[k])
            value = mix(low, [xp[i + 1, k + 2] for i in range(e)])
            if e + 1 < ITERS:
                xp[e + 1, k + 2] = value
            else:
                wl[3, k] = value

    def image(e, factor, weights):
        mix = mixer(e, factor, weights)

        def body(k, carry):
            for c in range(3):
                here = z1[c, k + 1]
                off = off_diagonal(z1[c, k], turn(here), z1[c, k + 2], k + 1)
                value = mix(xu[e, c, k + 1] - off, [xu[i + 1, c, k + 1] for i in range(e)])
                ss[e, c, k] = mix(y0[e, c, k + 2] + here, [ss[i, c, k] for i in range(e)])
                if e + 1 < ITERS:
                    xu[e + 1, c, k + 1] = value
                else:
                    wl[c, k] = value
            ss[e, 3, k] = mix(qs[e, k + 2], [ss[i, 3, k] for i in range(e)])
            return carry
        return body

    def held_of(i, c, k):
        if i > 0:
            return vv[i - 1, c, k]
        return xp[0, k + 2] if c == 3 else xu[0, c, k + 1]

    def image_of(e, c, k):
        if e + 1 == ITERS:
            return wl[c, k]
        return xp[e + 1, k + 2] if c == 3 else xu[e + 1, c, k + 1]

    stages[0].wait()
    pl.semaphore_wait(barrier, met)
    first_begin(0)
    first_copy(0, 0).start()
    spread(0)
    for item in stages[1:4]:
        item.wait()
    first_begin(1)
    first_copy(1, 0).start()
    first_copy(2, 0).start()
    stages[4].wait()
    first_begin(3)
    first_copy(3, 0).start()
    for item in own[1:4]:
        item.wait()
    first_near(1)
    first_near(2)
    loop(h, coefficients, low=1)
    loop(h, masses, low=1)
    further(1)
    own[0].wait()
    first_near(0)
    guess_own(0)
    first_far(0)

    zero = jnp.zeros((rows, nz), f32)
    inverses, entries = [], {}
    factor, weights = None, []
    for e in range(ITERS):
        if e > 0:
            arrive(6, e)
            arrive(0, e)
        guess_rest(e)
        loop(h, schur(e))
        begin(2, e)
        if e == 0:
            further(1)
            own[4].wait()
            first_near(3)
        velocity_share(e)
        begin(4, e)
        for k in range(1, h - 1):
            velocity_along(e, k)
        begin(3, e)
        loop(h, velocity_across(e))
        begin(5, e)
        second_across(e)
        low_own(e)
        if e == 0:
            first_far(1)
            coefficients(0, 0)
            coefficients(h + 1, 0)
            ca[0] = co[1, 0] * co[7, 0]
            ca[1] = co[0, h + 1] * co[7, h + 1]
            ca[2] = co[1, 1] * ca[0]
            ca[3] = co[0, h] * ca[1]
            first_far(3)
            further(1)
        else:
            sums = reduce_end(e - 1, e + 1)
            norm = jnp.sqrt(sums[0])
            factor = 1.0 / norm
            if e > 1:
                entries[(e - 1, e - 2)] = norm
            inverses.append(factor)
            weights = []
            for i in range(e):
                value = sums[i + 1] * inverses[i] * factor
                entries[(i, e - 1)] = value
                weights.append(value * inverses[i])

            def form(k, carry, e=e):
                for c in range(4):
                    value = image_of(e - 1, c, k) * factor
                    for i in range(e):
                        value = value - weights[i] * held_of(i, c, k)
                    vv[e - 1, c, k] = value
                return carry

            loop(h, form)
            hand_over(ITERS + e - 1)
            arrive(1, e)
        arrive(2, e)
        velocity_along(e, 0)
        velocity_along(e, h - 1)
        near_across(e)
        arrive(4, e)
        near_along(e)
        image_low(e, factor, weights)
        if e + 1 < ITERS:
            begin(6, e + 1)
        arrive(3, e)

        scale = factor if e > 0 else 1.0

        def beyond(c, e=e, scale=scale):
            return y0[e, c, 0] * scale, y0[e, c, h + 3] * scale

        below, above = beyond(0)
        if e + 1 < ITERS:
            xp[e + 1, 2] = xp[e + 1, 2] + 0.5 * (ca[0] * below)
            xp[e + 1, h + 1] = xp[e + 1, h + 1] - 0.5 * (ca[1] * above)
            begin(0, e + 1)
        else:
            wl[3, 0] = wl[3, 0] + 0.5 * (ca[0] * below)
            wl[3, h - 1] = wl[3, h - 1] - 0.5 * (ca[1] * above)
        second_edges(e, 1)
        second_edges(e, 2)
        loop(h, image(e, factor, weights))
        hand_over(e)
        if e == 0:
            further(len(steps))
        arrive(5, e)
        for c in range(3):
            below, above = beyond(c)
            if e + 1 < ITERS:
                xu[e + 1, c, 1] = xu[e + 1, c, 1] - ca[2] * below
                xu[e + 1, c, h] = xu[e + 1, c, h] - ca[3] * above
            else:
                wl[c, 0] = wl[c, 0] - ca[2] * below
                wl[c, h - 1] = wl[c, h - 1] - ca[3] * above
        if e + 1 == ITERS:
            hand_over(2 * ITERS - 1)

        if e + 1 < ITERS:
            begin(1, e + 1)

        def totals(k, acc, e=e):
            acc = list(acc)
            found = [image_of(e, c, k) for c in range(4)]
            for i in range(e + 1):
                held = [held_of(i, c, k) for c in range(4)]
                term = held[0] * found[0] + held[1] * found[1]
                acc[i + 1] = acc[i + 1] + (term + (held[2] * found[2] + held[3] * found[3]))
                if i == e:
                    term = held[0] * held[0] + held[1] * held[1]
                    acc[0] = acc[0] + (term + (held[2] * held[2] + held[3] * held[3]))
            if e + 1 == ITERS:
                term = found[0] * found[0] + found[1] * found[1]
                acc[e + 2] = acc[e + 2] + (term + (found[2] * found[2] + found[3] * found[3]))
            return tuple(acc)

        count = e + 2 if e + 1 < ITERS else e + 3
        reduce_start(e, loop(h, totals, (zero,) * count))
        if e + 1 < ITERS:
            guess_own(e + 1)

    for g in range(len(first)):
        first_finish(g)
    first_out.wait()
    for e in range(ITERS):
        for kind in range(7):
            if e > 0 or kind in (2, 3, 4, 5):
                finish(kind, e)
    for here, there in outs:
        here.wait()
        there.wait()
    for e in range(ITERS - 1):
        red_wait(e, red_send)
    sums = reduce_end(ITERS - 1, ITERS + 2)
    norm = jnp.sqrt(sums[0])
    factor = 1.0 / norm
    entries[(ITERS - 1, ITERS - 2)] = norm
    inverses.append(factor)
    left = sums[ITERS + 1] * factor * factor
    spread = []
    for i in range(ITERS):
        value = sums[i + 1] * inverses[i] * factor
        entries[(i, ITERS - 1)] = value
        spread.append(value * inverses[i])
        left = left - value * value
    norm = jnp.sqrt(left)
    entries[(ITERS, ITERS - 1)] = norm
    inverse = 1.0 / norm
    lines = inverses + [factor * inverse] + [g * inverse for g in spread]
    for i, value in enumerate(lines):
        scal[i : i + 1] = jnp.broadcast_to(value, (1, LANES))
    r = lax.broadcasted_iota(jnp.int32, (8, LANES), 0)
    c = lax.broadcasted_iota(jnp.int32, (8, LANES), 1)
    table = jnp.zeros((8, LANES), f32)
    for (i, j), value in entries.items():
        table = table + jnp.where(jnp.logical_and(r == i, c == j), value, 0.0)
    scal[8:16] = table
    red_wait(ITERS - 1, red_send)


def write(ob, os_, scal, basis, search, hess, bb, sb, hb, sems):
    def value(i):
        return scal[i : i + 1, 0:1]

    copies = []

    def emit(src, dst, i):
        item = pltpu.make_async_copy(src, dst, sems.at[i])
        item.start()
        copies.append(item)

    hb[...] = scal[8 : 8 + ITERS + 1, 0:ITERS]
    emit(hb, hess, 2 * ITERS + 1)
    planes = ob.shape[2]
    inverse = [value(i) for i in range(ITERS)]
    for e in range(ITERS):
        def body(k, carry, e=e):
            for c in range(4):
                bb[e, c, k] = ob[e, c, k] * inverse[e]
                sb[e, c, k] = os_[e, c, k] * inverse[e]
            return carry

        loop(planes, body)
        emit(bb.at[e], basis.at[e], e)
        emit(sb.at[e], search.at[e], ITERS + 1 + e)
    weights = [value(ITERS + i) for i in range(ITERS + 1)]

    def last(k, carry):
        for c in range(4):
            total = ob[ITERS, c, k] * weights[0]
            for i in range(ITERS):
                total = total - weights[i + 1] * ob[i, c, k]
            bb[ITERS, c, k] = total
        return carry

    loop(planes, last)
    emit(bb.at[ITERS], basis.at[ITERS], ITERS)
    for item in copies:
        item.wait()


def per_device(slabs, subs, start, wind, reaction, mass):
    _, cx, cy, nz = start.shape
    n = slabs * subs
    rows, h = subs * cy, cx // subs
    assert subs == 2 and cx % subs == 0 and h >= 3
    f32 = jnp.float32

    def field(*lead):
        return pltpu.VMEM((*lead, rows, nz), f32)

    anywhere = pl.BlockSpec(memory_space=pl.ANY)
    vmem = pl.BlockSpec(memory_space=pltpu.VMEM)
    hbm = pl.BlockSpec(memory_space=pltpu.HBM)
    ob, os_, scal = pl.pallas_call(
        functools.partial(kernel, slabs, subs, cx, cy, nz),
        out_shape=(
            jax.ShapeDtypeStruct((ITERS + 1, 4, cx, cy, nz), f32),
            jax.ShapeDtypeStruct((ITERS, 4, cx, cy, nz), f32),
            jax.ShapeDtypeStruct((16, LANES), f32),
        ),
        in_specs=[hbm] * 4,
        out_specs=(anywhere, anywhere, vmem),
        scratch_shapes=[
            pltpu.VMEM((9, cx, cy, nz), f32),
            field(ITERS, h + 4),
            field(ITERS, 3, h + 2),
            field(ITERS, h + 4),
            field(ITERS, 3, h + 4),
            field(ITERS, 2),
            field(h + 2),
            field(3, h + 2),
            field(5, h + 2),
            field(9, h + 2),
            field(4),
            field(4),
            field(ITERS - 1, 4, h),
            field(ITERS, 4, h),
            field(4, h),
            pltpu.VMEM((ITERS, n, 1, LANES), f32),
            pltpu.SemaphoreType.DMA((4, 3)),
            pltpu.SemaphoreType.DMA((4, 3)),
            pltpu.SemaphoreType.DMA((7, ITERS, 2)),
            pltpu.SemaphoreType.DMA((7, ITERS, 2)),
            pltpu.SemaphoreType.DMA((ITERS,)),
            pltpu.SemaphoreType.DMA((ITERS,)),
            pltpu.SemaphoreType.DMA((11,)),
            pltpu.SemaphoreType.DMA((2 * ITERS,)),
            pltpu.SemaphoreType.DMA((2 * ITERS,)),
            pltpu.SemaphoreType.DMA((2 * ITERS,)),
            pltpu.SemaphoreType.REGULAR(((slabs - 1).bit_length(), 2)),
        ],
        compiler_params=pltpu.CompilerParams(
            collective_id=0, has_side_effects=True, vmem_limit_bytes=40_000_000
        ),
    )(*(pltpu.with_memory_space_constraint(x, pltpu.HBM) for x in (start, wind, reaction, mass)))
    return pl.pallas_call(
        write,
        out_shape=(
            jax.ShapeDtypeStruct((ITERS + 1, 4, cx, cy, nz), f32),
            jax.ShapeDtypeStruct((ITERS, 4, cx, cy, nz), f32),
            jax.ShapeDtypeStruct((ITERS + 1, ITERS), f32),
        ),
        in_specs=[vmem] * 3,
        out_specs=(hbm, hbm, hbm),
        scratch_shapes=[
            pltpu.VMEM((ITERS + 1, 4, cx, cy, nz), f32),
            pltpu.VMEM((ITERS, 4, cx, cy, nz), f32),
            pltpu.VMEM((ITERS + 1, ITERS), f32),
            pltpu.SemaphoreType.DMA((2 * ITERS + 2,)),
        ],
        compiler_params=pltpu.CompilerParams(vmem_limit_bytes=10_000_000),
    )(ob, os_, scal)


def solution(mesh):
    slabs, subs = mesh.shape["slab"], mesh.shape["sub"]
    return jax.shard_map(
        functools.partial(per_device, slabs, subs),
        mesh=mesh,
        in_specs=(
            P(None, "slab", "sub", None),
            P(None, "slab", "sub", None),
            P("slab", "sub", None),
            P("slab", "sub", None),
        ),
        out_specs=(P(None, None, "slab", "sub", None), P(None, None, "slab", "sub", None), P()),
        check_vma=False,
    )
```

```python
import functools

import jax
import jax.numpy as jnp
from jax import lax
from jax.experimental import pallas as pl
from jax.experimental.pallas import tpu as pltpu
from jax.sharding import PartitionSpec as P

ITERS = 3
UNROLL = 6
LANES = 128
MESH = pl.DeviceIdType.MESH


def fold(x):
    rows, cols = x.shape
    total = None
    for r in range(0, rows, 8):
        for c in range(0, cols, LANES):
            piece = x[r : r + 8, c : c + LANES]
            total = piece if total is None else total + piece
    return total


def loop(count, body, init=0, low=0):
    step = max(u for u in range(1, UNROLL + 1) if count % u == 0)

    def several(k, carry):
        for i in range(step):
            carry = body(low + k * step + i, carry)
        return carry

    return lax.fori_loop(0, count // step, several, init)


def kernel(
    slabs, subs, cx, cy, nz,
    start, wind, reaction, mass, ob, os_, scal,
    stage, xp, xu, qs, y0, yq, t1, z1, raw, co, ca, mk, vv, ss, wl, red,
    init_send, init_recv, send, recv, red_send, red_recv, load, out_local, out_send, out_recv, known,
):
    slab, sub = lax.axis_index("slab"), lax.axis_index("sub")
    n = slabs * subs
    me = slab * subs + sub
    h = cx // subs
    rows = subs * cy
    f32 = jnp.float32
    other = 1 - sub
    has_left, has_right = me > 0, me < n - 1
    has_cross = jnp.where(sub == 0, slab, slabs - 1 - slab) > 0
    mine = pl.ds(pl.multiple_of(sub * cy, 8), cy)
    theirs = pl.ds(pl.multiple_of(other * cy, 8), cy)

    def staged(lo, count):
        return lambda planes: stage.at[pl.ds(lo, count), planes]

    first = [
        (lambda planes: stage.at[3, planes], lambda planes, lines: xp.at[0, planes, lines], 2, 2),
        (staged(4, 4), lambda planes, lines: raw.at[pl.ds(0, 4), planes, lines], 1, 1),
        (lambda planes: stage.at[8, planes], lambda planes, lines: raw.at[4, planes, lines], 1, 0),
        (staged(0, 3), lambda planes, lines: xu.at[0, :, planes, lines], 1, 1),
    ]

    def window(g, side):
        _, _, at, w = first[g]
        return pl.ds(side * (h - w), h + w), pl.ds(at - side * w, h + w)

    def local(g, src, dst, sem):
        a, b = window(g, sub)
        return pltpu.make_async_copy(src(a), dst(b), load.at[sem])

    stages = [
        pltpu.make_async_copy(start.at[3], stage.at[3], load.at[0]),
        pltpu.make_async_copy(wind, stage.at[pl.ds(4, 3)], load.at[1]),
        pltpu.make_async_copy(reaction, stage.at[7], load.at[2]),
        pltpu.make_async_copy(mass, stage.at[8], load.at[3]),
        pltpu.make_async_copy(start.at[pl.ds(0, 3)], stage.at[pl.ds(0, 3)], load.at[4]),
    ]
    own = [
        local(0, lambda a: start.at[3, a], lambda b: xp.at[0, b, mine], 5),
        local(1, lambda a: wind.at[:, a], lambda b: raw.at[pl.ds(0, 3), b, mine], 6),
        local(1, lambda a: reaction.at[a], lambda b: raw.at[3, b, mine], 7),
        local(2, lambda a: mass.at[a], lambda b: raw.at[4, b, mine], 8),
        local(3, lambda a: start.at[pl.ds(0, 3), a], lambda b: xu.at[0, :, b, mine], 9),
    ]
    first_out = pltpu.make_async_copy(start, ob.at[0], load.at[10])
    for item in stages:
        item.start()
    for item in own:
        item.start()

    barrier = pltpu.get_barrier_semaphore()

    def greet(sem, at, core):
        pl.semaphore_signal(sem, inc=1, device_id=(at, core), device_id_type=MESH)

    def near(way):
        for core in range(subs):
            greet(barrier, slab + way, core)

    greet(barrier, slab, other)
    pl.when(slab > 0)(lambda: near(-1))
    pl.when(slab < slabs - 1)(lambda: near(1))
    met = 1 + jnp.where(slab > 0, subs, 0) + jnp.where(slab < slabs - 1, subs, 0)
    steps = [1 << i for i in range((slabs - 1).bit_length())]

    def spread(i):
        d = steps[i]
        pl.when(slab + d < slabs)(lambda: greet(known.at[i, 0], slab + d, sub))
        pl.when(slab - d >= 0)(lambda: greet(known.at[i, 1], slab - d, sub))

    def gather(i):
        d = steps[i]
        pl.when(slab - d >= 0)(lambda: pl.semaphore_wait(known.at[i, 0], 1))
        pl.when(slab + d < slabs)(lambda: pl.semaphore_wait(known.at[i, 1], 1))

    def further(count):
        for _ in range(count):
            if pending:
                i = pending.pop(0)
                gather(i)
                if i + 1 < len(steps):
                    spread(i + 1)

    pending = list(range(len(steps)))

    def clear(low):
        def inner():
            zero = jnp.zeros((rows, nz), f32)
            for e in range(ITERS):
                for k in range(2):
                    xp[e, k if low else 2 + h + k] = zero
                qs[e, 1 if low else 2 + h] = zero
                y0[e, 0, 1 if low else 2 + h] = zero
                for c in range(3):
                    xu[e, c, 0 if low else 1 + h] = zero
                    y0[e, c, 0 if low else 3 + h] = zero
            for c in range(4):
                raw[c, 0 if low else 1 + h] = zero
        return inner

    pl.when(jnp.logical_not(has_left))(clear(True))
    pl.when(jnp.logical_not(has_right))(clear(False))

    row = lax.broadcasted_iota(jnp.int32, (rows, nz), 0)
    col = lax.broadcasted_iota(jnp.int32, (rows, nz), 1)
    mk[0] = jnp.where(row == rows - 1, 0.0, 1.0)
    mk[1] = jnp.where(row == 0, 0.0, 1.0)
    mk[2] = jnp.where(col == nz - 1, 0.0, 1.0)
    mk[3] = jnp.where(col == 0, 0.0, 1.0)

    def first_copy(g, kind):
        src, dst, at, w = first[g]
        if kind == 0:
            a, b = window(g, other)
            target, slot = (slab, other), 0
        elif kind == 1:
            a, b = pl.ds(cx - w, w), pl.ds(at - w, w)
            target, slot = (slab + 1, 0), 1 + sub
        else:
            a, b = pl.ds(0, w), pl.ds(at + h, w)
            target, slot = (slab - 1, subs - 1), 1 + sub
        if kind > 0 and g == 3:
            src = lambda planes: stage.at[pl.ds(1, 2), planes]
            dst = lambda planes, lines: xu.at[0, pl.ds(1, 2), planes, lines]
        return pltpu.make_async_remote_copy(
            src_ref=src(a), dst_ref=dst(b, mine), send_sem=init_send.at[g, kind],
            recv_sem=init_recv.at[g, slot], device_id=target, device_id_type=MESH,
        )

    def first_begin(g):
        if first[g][3] > 0:
            pl.when(slab < slabs - 1)(lambda: first_copy(g, 1).start())
            pl.when(slab > 0)(lambda: first_copy(g, 2).start())

    def first_wait(ref, sem):
        pltpu.make_async_copy(ref, ref, sem).wait()

    def first_near(g):
        _, dst, _, _ = first[g]
        _, b = window(g, sub)
        first_wait(dst(b, theirs), init_recv.at[g, 0])

    def first_far(g):
        _, dst, at, w = first[g]
        if g == 3:
            dst = lambda planes, lines: xu.at[0, pl.ds(1, 2), planes, lines]
        if w > 0:
            def inner():
                for r in range(subs):
                    first_wait(dst(pl.ds(0, w), pl.ds(r * cy, cy)), init_recv.at[g, 1 + r])
            pl.when(has_cross)(inner)

    def first_finish(g):
        first_copy(g, 0).wait_send()
        if first[g][3] > 0:
            pl.when(slab < slabs - 1)(lambda: first_copy(g, 1).wait_send())
            pl.when(slab > 0)(lambda: first_copy(g, 2).wait_send())

    def remote(kind, e, way):
        if kind == 0 or kind == 6:
            deep = kind // 6
            pair = (h + 1 - deep, 1 - deep) if way == 0 else (2 + deep, h + 2 + deep)
            src, dst = xp.at[e, pair[0]], xp.at[e, pair[1]]
        elif kind == 1:
            pair, pick = (h, 0) if way == 0 else (1, h + 1), pl.ds(1, 2)
            src, dst = xu.at[e, pick, pair[0]], xu.at[e, pick, pair[1]]
        elif kind == 2:
            pair = (h + 1, 1) if way == 0 else (2, h + 2)
            src, dst = qs.at[e, pair[0]], qs.at[e, pair[1]]
        elif kind == 4:
            src, dst = yq.at[e, way], y0.at[e, 0, 1 if way == 0 else h + 2]
        else:
            pair = (h, 0) if way == 0 else (3, h + 3)
            pick = 0 if kind == 3 else pl.ds(1, 2)
            src, dst = y0.at[e, pick, pair[0]], y0.at[e, pick, pair[1]]
        target = me + 1 if way == 0 else me - 1
        return pltpu.make_async_remote_copy(
            src_ref=src, dst_ref=dst, send_sem=send.at[kind, e, way], recv_sem=recv.at[kind, e, way],
            device_id=(target // subs, lax.rem(target, subs)), device_id_type=MESH,
        )

    def begin(kind, e):
        pl.when(has_right)(lambda: remote(kind, e, 0).start())
        pl.when(has_left)(lambda: remote(kind, e, 1).start())

    def arrive(kind, e):
        pl.when(has_left)(lambda: remote(kind, e, 0).wait_recv())
        pl.when(has_right)(lambda: remote(kind, e, 1).wait_recv())

    def finish(kind, e):
        pl.when(has_right)(lambda: remote(kind, e, 0).wait_send())
        pl.when(has_left)(lambda: remote(kind, e, 1).wait_send())

    lane = lax.broadcasted_iota(jnp.int32, (1, LANES), 1)

    def reduce_start(e, parts):
        line = jnp.zeros((1, LANES), f32)
        for i, part in enumerate(parts):
            line = line + jnp.where(lane == i, jnp.sum(fold(part), keepdims=True), 0.0)
        red[e, me] = line

        def tell(at, core):
            pltpu.make_async_remote_copy(
                src_ref=red.at[e, me], dst_ref=red.at[e, me],
                send_sem=red_send.at[e], recv_sem=red_recv.at[e],
                device_id=(at, core), device_id_type=MESH,
            ).start()

        def push(k, carry):
            at = lax.rem(slab + k, slabs)
            for core in range(subs):
                tell(at, core)
            return carry

        lax.fori_loop(1, slabs, push, 0)
        tell(slab, other)

    def red_wait(e, sem):
        block = red.at[e, pl.ds(0, n - 1)]
        pltpu.make_async_copy(block, block, sem.at[e]).wait()

    def reduce_end(e, count):
        red_wait(e, red_recv)
        total = jnp.sum(red[e], axis=0)
        return [
            jnp.sum(jnp.where(lane == i, total, 0.0), axis=1, keepdims=True)
            for i in range(count)
        ]

    def deliver(i, src, dst):
        planes = pl.ds(sub * h, h)
        return (
            pltpu.make_async_copy(src.at[:, :, mine], dst.at[:, planes], out_local.at[i]),
            pltpu.make_async_remote_copy(
                src_ref=src.at[:, :, theirs], dst_ref=dst.at[:, planes],
                send_sem=out_send.at[i], recv_sem=out_recv.at[i],
                device_id=(slab, other), device_id_type=MESH,
            ),
        )

    def results():
        return [deliver(e, ss.at[e], os_.at[e]) for e in range(ITERS)] + [
            deliver(ITERS + e, vv.at[e], ob.at[e + 1]) for e in range(ITERS - 1)
        ] + [deliver(2 * ITERS - 1, wl, ob.at[ITERS])]

    outs = results()

    def hand_over(i):
        for item in outs[i]:
            item.start()

    def turn(f):
        return (
            pltpu.roll(f, rows - 1, 0), pltpu.roll(f, 1, 0),
            pltpu.roll(f, nz - 1, 1), pltpu.roll(f, 1, 1),
        )

    def masked(f):
        yp, ym, zp, zm = turn(f)
        return yp * mk[0], ym * mk[1], zp * mk[2], zm * mk[3]

    def off_diagonal(below, around, above, k):
        yp, ym, zp, zm = around
        total = co[0, k] * above + co[1, k] * below
        total = total + (co[2, k] * yp + co[3, k] * ym)
        return total + (co[4, k] * zp + co[5, k] * zm)

    def inside(k):
        at = me * h + k
        return jnp.where(jnp.logical_and(at >= 0, at < n * h), 1.0, 0.0)

    def coefficients(k, carry):
        hx, hy, hz = 0.5 * raw[0, k], 0.5 * raw[1, k], 0.5 * raw[2, k]
        co[0, k] = 1.0 - hx
        co[1, k] = 1.0 + hx
        co[2, k] = (1.0 - hy) * mk[0]
        co[3, k] = (1.0 + hy) * mk[1]
        co[4, k] = (1.0 - hz) * mk[2]
        co[5, k] = (1.0 + hz) * mk[3]
        diagonal = 6.0 + raw[3, k]
        co[6, k] = diagonal
        co[7, k] = inside(k - 1) / diagonal
        return carry

    def masses(k, carry):
        co[8, k] = 1.0 / raw[4, k]
        return carry

    def guess_own(e):
        for k in range(1, h + 1):
            here = xp[e, k + 1]
            yp, ym, zp, zm = masked(here)
            total = (yp + ym) + (zp + zm)
            if k > 1:
                total = total + xp[e, k]
            if k < h:
                total = total + xp[e, k + 2]
            t1[k] = (here + total * (1.0 / 7.0)) * (1.0 / 7.0)

    def guess_rest(e):
        t1[1] = t1[1] + xp[e, 1] * (1.0 / 49.0)
        t1[h] = t1[h] + xp[e, h + 2] * (1.0 / 49.0)
        for k in (0, h + 1):
            guess(e)(k, 0)

    def guess(e):
        def body(k, carry):
            here = xp[e, k + 1]
            yp, ym, zp, zm = masked(here)
            total = (xp[e, k] + xp[e, k + 2]) + (yp + ym) + (zp + zm)
            t1[k] = (here + total * (1.0 / 7.0)) * (inside(k - 1) * (1.0 / 7.0))
            return carry
        return body

    def schur(e):
        def body(k, carry):
            here = t1[k + 1]
            off = off_diagonal(t1[k], turn(here), t1[k + 2], k + 1)
            qs[e, k + 2] = (off - co[6, k + 1] * here) * co[8, k + 1]
            return carry
        return body

    def velocity_along(e, k):
        found = xu[e, 0, k + 1] - 0.5 * (qs[e, k + 3] - qs[e, k + 1])
        y0[e, 0, k + 2] = found * co[7, k + 1]

    def velocity_across(e):
        def body(k, carry):
            yp, ym, zp, zm = masked(qs[e, k + 2])
            scale = co[7, k + 1]
            y0[e, 1, k + 2] = (xu[e, 1, k + 1] - 0.5 * (yp - ym)) * scale
            y0[e, 2, k + 2] = (xu[e, 2, k + 1] - 0.5 * (zp - zm)) * scale
            return carry
        return body

    def second(e, c, k, skip=None):
        yp, ym, zp, zm = turn(y0[e, c, k + 2])
        off = (co[2, k + 1] * yp + co[3, k + 1] * ym) + (co[4, k + 1] * zp + co[5, k + 1] * zm)
        if skip != 0:
            off = off + co[0, k + 1] * y0[e, c, k + 3]
        if skip != 1:
            off = off + co[1, k + 1] * y0[e, c, k + 1]
        z1[c, k + 1] = off * co[7, k + 1]

    def second_across(e):
        for c in (1, 2):
            for k in range(h):
                second(e, c, k, 1 if k == 0 else 0 if k == h - 1 else None)

    def across(e, k):
        one, two = y0[e, 1, k + 2] + z1[1, k + 1], y0[e, 2, k + 2] + z1[2, k + 1]
        a, b = pltpu.roll(one, rows - 1, 0), pltpu.roll(one, 1, 0)
        found = a * mk[0] - b * mk[1]
        a, b = pltpu.roll(two, nz - 1, 1), pltpu.roll(two, 1, 1)
        return 0.5 * (found + (a * mk[2] - b * mk[3]))

    def low_own(e):
        for k in range(h):
            q = qs[e, k + 2]
            yp, ym, zp, zm = masked(q)
            total = (yp + ym) + (zp + zm)
            if k > 0:
                total = total + qs[e, k + 1]
            if k < h - 1:
                total = total + qs[e, k + 3]
            total = 0.5 * total - 3.0 * q
            if 0 < k < h - 1:
                total = total - across(e, k)
            t1[k + 1] = total

    def velocity_share(e):
        yq[e, 0] = (xu[e, 0, h] + 0.5 * qs[e, h]) * co[7, h]
        yq[e, 1] = (xu[e, 0, 1] - 0.5 * qs[e, 3]) * co[7, 1]

    def near_across(e):
        for k in (-1, h):
            velocity_across(e)(k, 0)
        for c in (1, 2):
            z1[c, 1] = z1[c, 1] + co[1, 1] * y0[e, c, 1] * co[7, 1]
            z1[c, h] = z1[c, h] + co[0, h] * y0[e, c, h + 2] * co[7, h]
        for k in range(h):
            second(e, 0, k, 1 if k == 0 else 0 if k == h - 1 else None)
        t1[1] = t1[1] + 0.5 * qs[e, 1] - across(e, 0)
        t1[h] = t1[h] + 0.5 * qs[e, h + 2] - across(e, h - 1)

    def near_along(e):
        for k, near, sign in ((-1, 2, -0.5), (h, h + 1, 0.5)):
            y0[e, 0, k + 2] = y0[e, 0, k + 2] + (sign * qs[e, near]) * co[7, k + 1]
        z1[0, 1] = z1[0, 1] + co[1, 1] * y0[e, 0, 1] * co[7, 1]
        z1[0, h] = z1[0, h] + co[0, h] * y0[e, 0, h + 2] * co[7, h]
        second_edges(e, 0)

    def second_edges(e, c):
        second(e, c, -1, 1)
        second(e, c, h, 0)

    def mixer(e, factor, weights):
        def mix(value, held):
            if e > 0:
                value = value * factor
                for g, item in zip(weights, held):
                    value = value - g * item
            return value
        return mix

    def image_low(e, factor, weights):
        mix = mixer(e, factor, weights)
        full = [y0[e, 0, k + 2] + z1[0, k + 1] for k in range(-1, h + 1)]
        for k in range(h):
            low = t1[k + 1] - 0.5 * (full[k + 2] - full[k])
            value = mix(low, [xp[i + 1, k + 2] for i in range(e)])
            if e + 1 < ITERS:
                xp[e + 1, k + 2] = value
            else:
                wl[3, k] = value

    def image(e, factor, weights):
        mix = mixer(e, factor, weights)

        def body(k, carry):
            for c in range(3):
                here = z1[c, k + 1]
                off = off_diagonal(z1[c, k], turn(here), z1[c, k + 2], k + 1)
                value = mix(xu[e, c, k + 1] - off, [xu[i + 1, c, k + 1] for i in range(e)])
                ss[e, c, k] = mix(y0[e, c, k + 2] + here, [ss[i, c, k] for i in range(e)])
                if e + 1 < ITERS:
                    xu[e + 1, c, k + 1] = value
                else:
                    wl[c, k] = value
            ss[e, 3, k] = mix(qs[e, k + 2], [ss[i, 3, k] for i in range(e)])
            return carry
        return body

    def held_of(i, c, k):
        if i > 0:
            return vv[i - 1, c, k]
        return xp[0, k + 2] if c == 3 else xu[0, c, k + 1]

    def image_of(e, c, k):
        if e + 1 == ITERS:
            return wl[c, k]
        return xp[e + 1, k + 2] if c == 3 else xu[e + 1, c, k + 1]

    stages[0].wait()
    pl.semaphore_wait(barrier, met)
    first_begin(0)
    first_copy(0, 0).start()
    spread(0)
    for item in stages[1:4]:
        item.wait()
    first_begin(1)
    first_copy(1, 0).start()
    first_copy(2, 0).start()
    stages[4].wait()
    first_begin(3)
    first_copy(3, 0).start()
    for item in own[1:4]:
        item.wait()
    first_near(1)
    first_near(2)
    loop(h, coefficients, low=1)
    loop(h, masses, low=1)
    further(1)
    own[0].wait()
    first_out.start()
    first_near(0)
    guess_own(0)
    first_far(0)

    zero = jnp.zeros((rows, nz), f32)
    inverses, entries = [], {}
    factor, weights = None, []
    for e in range(ITERS):
        if e > 0:
            arrive(6, e)
            arrive(0, e)
        guess_rest(e)
        loop(h, schur(e))
        begin(2, e)
        if e == 0:
            further(1)
            own[4].wait()
            first_near(3)
        velocity_share(e)
        begin(4, e)
        for k in range(1, h - 1):
            velocity_along(e, k)
        begin(3, e)
        loop(h, velocity_across(e))
        begin(5, e)
        second_across(e)
        low_own(e)
        if e == 0:
            first_far(1)
            coefficients(0, 0)
            coefficients(h + 1, 0)
            ca[0] = co[1, 0] * co[7, 0]
            ca[1] = co[0, h + 1] * co[7, h + 1]
            ca[2] = co[1, 1] * ca[0]
            ca[3] = co[0, h] * ca[1]
            first_far(3)
            further(1)
        else:
            sums = reduce_end(e - 1, e + 1)
            norm = jnp.sqrt(sums[0])
            factor = 1.0 / norm
            if e > 1:
                entries[(e - 1, e - 2)] = norm
            inverses.append(factor)
            weights = []
            for i in range(e):
                value = sums[i + 1] * inverses[i] * factor
                entries[(i, e - 1)] = value
                weights.append(value * inverses[i])

            def form(k, carry, e=e):
                for c in range(4):
                    value = image_of(e - 1, c, k) * factor
                    for i in range(e):
                        value = value - weights[i] * held_of(i, c, k)
                    vv[e - 1, c, k] = value
                return carry

            loop(h, form)
            arrive(1, e)
        arrive(2, e)
        velocity_along(e, 0)
        velocity_along(e, h - 1)
        near_across(e)
        arrive(4, e)
        near_along(e)
        image_low(e, factor, weights)
        if e + 1 < ITERS:
            begin(6, e + 1)
        arrive(3, e)

        scale = factor if e > 0 else 1.0

        def beyond(c, e=e, scale=scale):
            return y0[e, c, 0] * scale, y0[e, c, h + 3] * scale

        below, above = beyond(0)
        if e + 1 < ITERS:
            xp[e + 1, 2] = xp[e + 1, 2] + 0.5 * (ca[0] * below)
            xp[e + 1, h + 1] = xp[e + 1, h + 1] - 0.5 * (ca[1] * above)
            begin(0, e + 1)
        else:
            wl[3, 0] = wl[3, 0] + 0.5 * (ca[0] * below)
            wl[3, h - 1] = wl[3, h - 1] - 0.5 * (ca[1] * above)
        second_edges(e, 1)
        second_edges(e, 2)
        loop(h, image(e, factor, weights))
        if e == 0:
            further(len(steps))
        arrive(5, e)
        for c in range(3):
            below, above = beyond(c)
            if e + 1 < ITERS:
                xu[e + 1, c, 1] = xu[e + 1, c, 1] - ca[2] * below
                xu[e + 1, c, h] = xu[e + 1, c, h] - ca[3] * above
            else:
                wl[c, 0] = wl[c, 0] - ca[2] * below
                wl[c, h - 1] = wl[c, h - 1] - ca[3] * above
        if e + 1 < ITERS:
            begin(1, e + 1)

        def totals(k, acc, e=e):
            acc = list(acc)
            found = [image_of(e, c, k) for c in range(4)]
            for i in range(e + 1):
                held = [held_of(i, c, k) for c in range(4)]
                term = held[0] * found[0] + held[1] * found[1]
                acc[i + 1] = acc[i + 1] + (term + (held[2] * found[2] + held[3] * found[3]))
                if i == e:
                    term = held[0] * held[0] + held[1] * held[1]
                    acc[0] = acc[0] + (term + (held[2] * held[2] + held[3] * held[3]))
            if e + 1 == ITERS:
                term = found[0] * found[0] + found[1] * found[1]
                acc[e + 2] = acc[e + 2] + (term + (found[2] * found[2] + found[3] * found[3]))
            return tuple(acc)

        count = e + 2 if e + 1 < ITERS else e + 3
        reduce_start(e, loop(h, totals, (zero,) * count))
        if e + 1 < ITERS:
            guess_own(e + 1)

    for i in range(2 * ITERS):
        hand_over(i)
    for g in range(len(first)):
        first_finish(g)
    first_out.wait()
    for e in range(ITERS):
        for kind in range(7):
            if e > 0 or kind in (2, 3, 4, 5):
                finish(kind, e)
    for here, there in outs:
        here.wait()
        there.wait()
    for e in range(ITERS - 1):
        red_wait(e, red_send)
    sums = reduce_end(ITERS - 1, ITERS + 2)
    norm = jnp.sqrt(sums[0])
    factor = 1.0 / norm
    entries[(ITERS - 1, ITERS - 2)] = norm
    inverses.append(factor)
    left = sums[ITERS + 1] * factor * factor
    spread = []
    for i in range(ITERS):
        value = sums[i + 1] * inverses[i] * factor
        entries[(i, ITERS - 1)] = value
        spread.append(value * inverses[i])
        left = left - value * value
    norm = jnp.sqrt(left)
    entries[(ITERS, ITERS - 1)] = norm
    inverse = 1.0 / norm
    lines = inverses + [factor * inverse] + [g * inverse for g in spread]
    for i, value in enumerate(lines):
        scal[i : i + 1] = jnp.broadcast_to(value, (1, LANES))
    r = lax.broadcasted_iota(jnp.int32, (8, LANES), 0)
    c = lax.broadcasted_iota(jnp.int32, (8, LANES), 1)
    table = jnp.zeros((8, LANES), f32)
    for (i, j), value in entries.items():
        table = table + jnp.where(jnp.logical_and(r == i, c == j), value, 0.0)
    scal[8:16] = table
    red_wait(ITERS - 1, red_send)


def write(ob, os_, scal, basis, search, hess, bb, sb, hb, sems):
    def value(i):
        return scal[i : i + 1, 0:1]

    copies = []

    def emit(src, dst, i):
        item = pltpu.make_async_copy(src, dst, sems.at[i])
        item.start()
        copies.append(item)

    hb[...] = scal[8 : 8 + ITERS + 1, 0:ITERS]
    emit(hb, hess, 2 * ITERS + 1)
    planes = ob.shape[2]
    inverse = [value(i) for i in range(ITERS)]
    for e in range(ITERS):
        def body(k, carry, e=e):
            for c in range(4):
                bb[e, c, k] = ob[e, c, k] * inverse[e]
                sb[e, c, k] = os_[e, c, k] * inverse[e]
            return carry

        loop(planes, body)
        emit(bb.at[e], basis.at[e], e)
        emit(sb.at[e], search.at[e], ITERS + 1 + e)
    weights = [value(ITERS + i) for i in range(ITERS + 1)]

    def last(k, carry):
        for c in range(4):
            total = ob[ITERS, c, k] * weights[0]
            for i in range(ITERS):
                total = total - weights[i + 1] * ob[i, c, k]
            bb[ITERS, c, k] = total
        return carry

    loop(planes, last)
    emit(bb.at[ITERS], basis.at[ITERS], ITERS)
    for item in copies:
        item.wait()


def per_device(slabs, subs, start, wind, reaction, mass):
    _, cx, cy, nz = start.shape
    n = slabs * subs
    rows, h = subs * cy, cx // subs
    assert subs == 2 and cx % subs == 0 and h >= 3
    f32 = jnp.float32

    def field(*lead):
        return pltpu.VMEM((*lead, rows, nz), f32)

    anywhere = pl.BlockSpec(memory_space=pl.ANY)
    vmem = pl.BlockSpec(memory_space=pltpu.VMEM)
    hbm = pl.BlockSpec(memory_space=pltpu.HBM)
    ob, os_, scal = pl.pallas_call(
        functools.partial(kernel, slabs, subs, cx, cy, nz),
        out_shape=(
            jax.ShapeDtypeStruct((ITERS + 1, 4, cx, cy, nz), f32),
            jax.ShapeDtypeStruct((ITERS, 4, cx, cy, nz), f32),
            jax.ShapeDtypeStruct((16, LANES), f32),
        ),
        in_specs=[hbm] * 4,
        out_specs=(anywhere, anywhere, vmem),
        scratch_shapes=[
            pltpu.VMEM((9, cx, cy, nz), f32),
            field(ITERS, h + 4),
            field(ITERS, 3, h + 2),
            field(ITERS, h + 4),
            field(ITERS, 3, h + 4),
            field(ITERS, 2),
            field(h + 2),
            field(3, h + 2),
            field(5, h + 2),
            field(9, h + 2),
            field(4),
            field(4),
            field(ITERS - 1, 4, h),
            field(ITERS, 4, h),
            field(4, h),
            pltpu.VMEM((ITERS, n, 1, LANES), f32),
            pltpu.SemaphoreType.DMA((4, 3)),
            pltpu.SemaphoreType.DMA((4, 3)),
            pltpu.SemaphoreType.DMA((7, ITERS, 2)),
            pltpu.SemaphoreType.DMA((7, ITERS, 2)),
            pltpu.SemaphoreType.DMA((ITERS,)),
            pltpu.SemaphoreType.DMA((ITERS,)),
            pltpu.SemaphoreType.DMA((11,)),
            pltpu.SemaphoreType.DMA((2 * ITERS,)),
            pltpu.SemaphoreType.DMA((2 * ITERS,)),
            pltpu.SemaphoreType.DMA((2 * ITERS,)),
            pltpu.SemaphoreType.REGULAR(((slabs - 1).bit_length(), 2)),
        ],
        compiler_params=pltpu.CompilerParams(
            collective_id=0, has_side_effects=True, vmem_limit_bytes=40_000_000
        ),
    )(*(pltpu.with_memory_space_constraint(x, pltpu.HBM) for x in (start, wind, reaction, mass)))
    return pl.pallas_call(
        write,
        out_shape=(
            jax.ShapeDtypeStruct((ITERS + 1, 4, cx, cy, nz), f32),
            jax.ShapeDtypeStruct((ITERS, 4, cx, cy, nz), f32),
            jax.ShapeDtypeStruct((ITERS + 1, ITERS), f32),
        ),
        in_specs=[vmem] * 3,
        out_specs=(hbm, hbm, hbm),
        scratch_shapes=[
            pltpu.VMEM((ITERS + 1, 4, cx, cy, nz), f32),
            pltpu.VMEM((ITERS, 4, cx, cy, nz), f32),
            pltpu.VMEM((ITERS + 1, ITERS), f32),
            pltpu.SemaphoreType.DMA((2 * ITERS + 2,)),
        ],
        compiler_params=pltpu.CompilerParams(vmem_limit_bytes=10_000_000),
    )(ob, os_, scal)


def solution(mesh):
    slabs, subs = mesh.shape["slab"], mesh.shape["sub"]
    return jax.shard_map(
        functools.partial(per_device, slabs, subs),
        mesh=mesh,
        in_specs=(
            P(None, "slab", "sub", None),
            P(None, "slab", "sub", None),
            P("slab", "sub", None),
            P("slab", "sub", None),
        ),
        out_specs=(P(None, None, "slab", "sub", None), P(None, None, "slab", "sub", None), P()),
        check_vma=False,
    )
```
